128 devices in a mesh: row: 16 (over y, x), col: 8 (over z, core).
Axes of the slice: x: 4, y: 4, z: 4, core: 2. Of those that a mesh axis runs over, the one named last changes fastest.
Arguments:
- a_window: float32 [16384, 8192], P('row', 'col'), may hold values from -6 to 6
- l_panel: float32 [16384, 1024], P('row'), may hold values from -0.1875 to 0.1875
- l_inverse: float32 [2, 512, 512], replicated, may hold values from -2 to 2, as said below
Outputs:
- reduced: float32 [16384, 8192], P('row', 'col')
The draws below stay inside these ranges and needn't reach their ends.
Inputs may be any that keep to these rules, and one draw needn't show every extreme that they name: `l_inverse`: both blocks are lower triangular, with diagonal entries between 0.5 and 2.
All inputs are finite; a program needn't handle non-finite values.
Results may differ from the reference program's by a relative error of at most 0.000067.
Values sent between devices are 32-bit elements; how exact they have to be, the bound alone decides.
A program may use at most 128 MiB of HBM per device.

```python
import jax
import jax.numpy as jnp
from jax import lax

N = 16384
B = 512
WC = 8192


def draw_l_inverse(key, part):
    first_key, second_key = jax.random.split(jax.random.fold_in(key, 17))
    spread = jnp.clip(jax.random.normal(first_key, (2, B, B), jnp.float32), -4.0, 4.0)
    diagonal = jax.random.uniform(second_key, (2, B), jnp.float32, 0.5, 1.5)
    strict = jnp.tril(spread, -1) / jnp.sqrt(jnp.float32(B))
    return strict + diagonal[:, :, None] * jnp.eye(B, dtype=jnp.float32)[None, :, :]


def shard_levels(own_key, extent, pieces, least, top_value):
    level, own = 1.0, jax.random.fold_in(own_key, 6)
    for axis_at, shards_of in pieces:
        steps = jnp.exp(jax.random.uniform(jax.random.fold_in(own, axis_at), (shards_of,), jnp.float32, least / len(pieces), top_value / len(pieces)))
        level = level * jnp.repeat(steps, extent[axis_at] // shards_of).reshape([-1 if axis == axis_at else 1 for axis in range(len(extent))])
    return level


def noise(own_key, shape, deviation, reach, cuts=(), kind=jnp.bfloat16):
    loudness = shard_levels(own_key, shape, cuts, -0.22, 0.18) if cuts else 1.0
    drawn = jax.random.normal(own_key, shape, jnp.float32) * deviation * loudness
    return jnp.minimum(jnp.maximum(drawn, -reach), reach).astype(kind)


def setup_inputs(seed: int = 0) -> dict:
    key_list = jax.random.split(jax.random.key(seed), 4)
    a_window = noise(key_list[0], (N, WC), 1.0, 6.0, ((0, 16), (1, 8)), jnp.float32)
    l_panel = noise(key_list[1], (N, 2 * B), (2 * B) ** -0.5, 0.1875, ((0, 16),), jnp.float32)
    l_inverse = draw_l_inverse(jax.random.fold_in(key_list[3], 71), 0)
    return {"a_window": a_window, "l_panel": l_panel, "l_inverse": l_inverse}


def matmul_hp(left, right):
    return jnp.dot(left, right, precision=lax.Precision.HIGHEST, preferred_element_type=jnp.float32)


def reference(a_window, l_panel, l_inverse):
    first_inv = l_inverse[0]
    second_inv = l_inverse[1]
    coupling = l_panel[B:2 * B, :B]
    leading = matmul_hp(a_window[:, :B], first_inv.T)
    second_col = matmul_hp(a_window[:, B:2 * B] - matmul_hp(leading, coupling.T), second_inv.T)
    solved = jnp.concatenate([leading, second_col], 1)
    upper_tile = matmul_hp(first_inv, solved[:B])
    lower_tile = matmul_hp(second_inv, solved[B:2 * B] - matmul_hp(coupling, upper_tile))
    diag_block = jnp.concatenate([upper_tile, lower_tile], 0)
    below = l_panel[2 * B:]
    product = matmul_hp(below, diag_block)
    reduced_g = solved[2 * B:] - 0.5 * product
    lower_panel = solved[2 * B:] - product
    width_left = WC - 2 * B
    update = a_window[2 * B:, 2 * B:] - matmul_hp(below, reduced_g[:width_left].T) - matmul_hp(reduced_g, below[:width_left].T)
    upper_rows = jnp.concatenate([diag_block, a_window[:2 * B, 2 * B:]], 1)
    lower_rows = jnp.concatenate([lower_panel, update], 1)
    return jnp.concatenate([upper_rows, lower_rows], 0)
```

```python
import jax
import jax.numpy as jnp
from jax import lax
from jax.experimental import pallas as pl
from jax.experimental.pallas import tpu as pltpu
from jax.sharding import PartitionSpec as P

MESH = pl.DeviceIdType.MESH
F32 = jnp.float32
BF16 = jnp.bfloat16

W = 1024
HB = 512
RC = 8
KT = W // (4 * RC)
RP = 16
KP = W // (4 * RP)
RL = 32
KL = HB // (4 * RL)
ZR = 16
KZ = HB // ZR
KZL = HB // 2 // RL
SIG = 4
SZ = 3
S1 = 12
ZL0 = 32
ZG0 = 50
DEEP = 6


def split(v):
    hi = v.astype(BF16)
    return hi, (v - hi.astype(F32)).astype(BF16)


def nn(a, b):
    return jnp.dot(a, b, preferred_element_type=F32)


def nt(a, b):
    return lax.dot_general(a, b, (((1,), (1,)), ((), ())), preferred_element_type=F32)


def mul3(op, a, b):
    return op(a[0], b[0]) + (op(a[0], b[1]) + op(a[1], b[0]))


def wrap(v):
    return lax.rem(v + 4, 4)


class Tree:
    def __init__(self, t, x, y, root):
        rx, ry = lax.rem(root, 4), lax.div(root, 4)
        sgn = 1 if t % 2 == 0 else -1
        dx, dy = wrap((x - rx) * sgn), wrap((y - ry) * sgn)
        main, sec = (dx, dy) if t < 2 else (dy, dx)
        self.depth = jnp.where(main == 0, jnp.where(sec == 0, 0, sec + 2), main + sec)
        self.root = jnp.logical_and(main == 0, sec == 0)
        step = jnp.where(sec == 0, sgn, -sgn)
        self.has = (
            jnp.logical_or(
                jnp.logical_and(sec == 0, main < 3), jnp.logical_and(sec > 0, main == 1)
            ),
            jnp.logical_and(main >= 1, sec < 3),
        )
        if t < 2:
            self.to = (y * 4 + wrap(x + step), wrap(y + sgn) * 4 + x)
        else:
            self.to = (wrap(y + step) * 4 + x, y * 4 + wrap(x + sgn))


def kernel(
    a_hbm, l_hbm, inv_hbm, o_hbm,
    big, u, lr, inv, l10, gbuf, ph, plo, ah, al, lh, ll, ih, il, lth, ltl,
    load_sem, tree_recv, tree_send, l10_send,
    zr1, zr2, lr1, lr2, gr1, gr2, zsend, out_sem,
):
    row, col = lax.axis_index("row"), lax.axis_index("col")
    x, y = lax.rem(row, 4), lax.div(row, 4)
    z, core = lax.div(col, 2), lax.rem(col, 2)
    other = col + 1 - 2 * core
    top = row == 0

    def remote(src, dst, send, recv, to):
        return pltpu.make_async_remote_copy(
            src_ref=src, dst_ref=dst, send_sem=send, recv_sem=recv,
            device_id=to, device_id_type=MESH,
        )

    def rows_of(ref, at, n):
        return ref.at[pl.ds(pl.multiple_of(at, 8), n)]

    load_inv = pltpu.make_async_copy(inv_hbm, inv, load_sem.at[0])
    load_l = pltpu.make_async_copy(l_hbm, lr, load_sem.at[1])
    load_inv.start()
    load_l.start()

    barrier = pltpu.get_barrier_semaphore()
    peers = [
        (y * 4 + wrap(x + 1), col), (y * 4 + wrap(x - 1), col),
        (wrap(y + 1) * 4 + x, col), (wrap(y - 1) * 4 + x, col),
        (row, other),
        (row, 2 * wrap(z + 1) + core), (row, 2 * wrap(z - 1) + core),
        (row, 2 * wrap(z + jnp.where(core == 0, -1, 1)) + 1 - core),
    ]
    for peer in peers:
        pl.semaphore_signal(barrier, inc=1, device_id=peer, device_id_type=MESH)
    pl.semaphore_wait(barrier, len(peers))

    trees = [Tree(t, x, y, col) for t in range(4)]

    def split_inverse():
        load_inv.wait()
        for b in range(2):
            h, l = split(inv[b])
            ih[b] = h
            il[b] = l

    def split_coupling():
        h, l = split(l10[...])
        lth[...] = h
        ltl[...] = l

    def tree_step(t, k, at, buf, n, send):
        tree = trees[t]
        ref = rows_of(buf, at, n)

        @pl.when(jnp.logical_not(tree.root))
        def _():
            remote(ref, ref, send.at[t, 0], tree_recv.at[t, k], (row, col)).wait_recv()

        for s in range(2):
            @pl.when(tree.has[s])
            def _():
                remote(ref, ref, send.at[t, s], tree_recv.at[t, k], (tree.to[s], col)).start()

    def p_rows(at, n, eye):
        rows = pl.ds(pl.multiple_of(at, 8), n)
        l0, l1 = lr[rows, :HB], lr[rows, HB:]
        if eye:
            i = at + lax.broadcasted_iota(jnp.int32, (n, HB), 0)
            j = lax.broadcasted_iota(jnp.int32, (n, HB), 1)
            l0 = jnp.where(top, jnp.where(i == j, 1.0, 0.0), l0)
            l1 = jnp.where(top, jnp.where(i == j + HB, 1.0, 0.0), l1)
        p1 = split(mul3(nn, split(l1), (ih[1], il[1])))
        ph[rows, HB:] = p1[0]
        plo[rows, HB:] = p1[1]
        p0 = split(
            mul3(nn, split(l0 - mul3(nn, p1, (lth[...], ltl[...]))), (ih[0], il[0]))
        )
        ph[rows, :HB] = p0[0]
        plo[rows, :HB] = p0[1]

    def right_solve(r, put):
        x0 = mul3(nt, split(r[:, :HB]), (ih[0], il[0]))
        put(0, x0)
        mid = r[:, HB:] - mul3(nt, split(x0), (lth[...], ltl[...]))
        put(HB, mul3(nt, split(mid), (ih[1], il[1])))

    @pl.when(col == 0)
    def _():
        load_a = pltpu.make_async_copy(a_hbm, big.at[pl.ds(2 * W, W)], load_sem.at[2])
        load_a.start()
        load_c = pltpu.make_async_copy(
            l_hbm.at[pl.ds(HB, HB), pl.ds(0, HB)], l10, load_sem.at[3]
        )
        load_t = pltpu.make_async_copy(a_hbm, big.at[pl.ds(0, W)], load_sem.at[4])

        @pl.when(top)
        def _():
            load_c.start()
            load_t.start()
            load_c.wait()
            load_t.wait()

        load_a.wait()

        def send_a(k, _):
            for half, to in ((0, 2), (1, 7)):
                src = rows_of(big, 2 * W + half * HB + k * ZR, ZR)
                at = jnp.where(2 * to == 0, 0, 0) + 2 * W
                root = row == to
                dst = rows_of(big, jnp.where(root, W, at) + half * HB + k * ZR, ZR)
                remote(src, dst, zsend.at[0, half], zr1.at[k], (row, to)).start()

            @pl.when(row == 1)
            def _():
                for half, recv in ((0, zr2), (1, zr1)):
                    src = rows_of(big, 2 * W + half * HB + k * ZR, ZR)
                    dst = rows_of(big, W + half * HB + k * ZR, ZR)
                    remote(src, dst, zsend.at[0, 2 + half], recv.at[k], (row, 1)).start()
            return 0

        lax.fori_loop(0, KZ, send_a, 0)
        split_inverse()
        load_l.wait()

        def slot(s):
            for t in range(4):
                k = s - SIG * trees[t].depth

                @pl.when(jnp.logical_and(k >= 0, k < KL))
                def _():
                    tree_step(t, k, (k * 4 + t) * RL, l10, RL, l10_send)

                k2 = k - KL

                @pl.when(jnp.logical_and(k2 >= 0, k2 < KP))
                def _():
                    tree_step(t, k2 + KL, (k2 * 4 + t) * RP, big, RP, tree_send)

        first = KL + SIG * DEEP

        def comm_only(s, _):
            slot(s)
            return 0

        lax.fori_loop(0, first, comm_only, 0)

        def send_l(k, _):
            for half, to in ((0, 2), (1, 7)):
                ref = rows_of(l10, half * (HB // 2) + k * RL, RL)
                remote(ref, ref, zsend.at[1, half], lr1.at[k], (row, to)).start()
            for half, recv in ((0, lr2), (1, lr1)):
                ref = rows_of(l10, half * (HB // 2) + k * RL, RL)
                remote(ref, ref, zsend.at[1, 2 + half], recv.at[k], (row, 1)).start()
            return 0

        lax.fori_loop(0, KZL, send_l, 0)
        split_coupling()

        def with_p(i, _):
            slot(first + i)
            p_rows(i * 128, 128, True)
            return 0

        lax.fori_loop(0, 8, with_p, 0)
        lax.fori_loop(first + 8, KL + KP + SIG * DEEP, comm_only, 0)

        def split_a(i, _):
            rows = pl.ds(pl.multiple_of(i * 128, 128), 128)
            h, l = split(big[rows])
            ah[rows] = h
            al[rows] = l
            return 0

        lax.fori_loop(0, 8, split_a, 0)

        def block(g, _):
            half, q = lax.rem(g, 2), lax.div(g, 2)
            at = half * HB + q * 128
            rows = pl.ds(pl.multiple_of(at, 128), 128)
            p = (ph[rows], plo[rows])
            for n in range(2):
                cols = slice(n * HB, n * HB + HB)
                e = mul3(nn, p, (ah[:, cols], al[:, cols]))
                f = mul3(nt, p, (ah[cols], al[cols]))
                a = big[pl.ds(pl.multiple_of(2 * W + at, 128), 128), cols]
                u[rows, cols] = jnp.where(top, e, a - e)
                gbuf[rows, cols] = a - 0.5 * (e + f)

            def put_g(c0, v):
                gbuf[rows, c0:c0 + HB] = v

            right_solve(gbuf[rows], put_g)

            def put_o(c0, v):
                u[rows, c0:c0 + HB] = v

            right_solve(u[rows], put_o)

            def send_g(j, _):
                ref = rows_of(gbuf, at + j * ZR, ZR)
                k = q * (128 // ZR) + j

                @pl.when(half == 0)
                def _():
                    remote(ref, ref, zsend.at[2, 0], gr1.at[k], (row, 2)).start()
                    remote(ref, ref, zsend.at[2, 2], gr2.at[k], (row, 1)).start()

                @pl.when(half == 1)
                def _():
                    remote(ref, ref, zsend.at[2, 1], gr1.at[k], (row, 7)).start()
                    remote(ref, ref, zsend.at[2, 3], gr1.at[k], (row, 1)).start()
                return 0

            lax.fori_loop(0, 128 // ZR, send_g, 0)
            return 0

        lax.fori_loop(0, 8, block, 0)

        for t in range(4):
            for s in range(2):
                @pl.when(trees[t].has[s])
                def _():
                    ref = l10.at[pl.ds(0, KL * RL)]
                    remote(ref, ref, l10_send.at[t, s], lr1.at[0], (row, 1)).wait_send()
                    ref = big.at[pl.ds(0, KP * RP)]
                    remote(ref, ref, tree_send.at[t, s], lr1.at[0], (row, 1)).wait_send()
        for s in range(4):
            ref = big.at[pl.ds(0, HB)]
            if s < 2:
                remote(ref, ref, zsend.at[0, s], lr1.at[0], (row, 1)).wait_send()
            else:
                @pl.when(row == 1)
                def _():
                    remote(ref, ref, zsend.at[0, s], lr1.at[0], (row, 1)).wait_send()
            remote(ref, ref, zsend.at[2, s], lr1.at[0], (row, 1)).wait_send()
            ref = l10.at[pl.ds(0, HB // 2)]
            remote(ref, ref, zsend.at[1, s], lr1.at[0], (row, 1)).wait_send()

    @pl.when(col > 0)
    def _():
        load_u = pltpu.make_async_copy(a_hbm, u, load_sem.at[2])
        load_u.start()
        mine = row == col
        load_r = pltpu.make_async_copy(l_hbm, big.at[pl.ds(0, W)], load_sem.at[4])

        @pl.when(mine)
        def _():
            load_r.start()
            load_r.wait()

        start = jnp.where(col == 1, S1, 0)
        far = z > 0
        first_depth = jnp.where(far, jnp.where(core == 0, z, 4 - z), 1)
        second_depth = jnp.where(far, jnp.where(core == 0, 5 - z, z + 1), 1)
        on = jnp.where(core == 0, jnp.logical_and(far, z < 3), z > 1)
        nxt = jnp.where(core == 0, col + 2, col - 2)
        half = jnp.where(core == 0, 0, 1)

        def z_step(s, begin, count, ref_of, first, second, kind, only_root):
            k = s - begin - SZ * first_depth

            @pl.when(jnp.logical_and(k >= 0, k < count))
            def _():
                def go():
                    src = ref_of(col, half, k)
                    remote(src, src, zsend.at[kind, 0], first.at[k], (row, col)).wait_recv()

                    @pl.when(on)
                    def _():
                        remote(
                            src, ref_of(nxt, half, k), zsend.at[kind, 0], first.at[k], (row, nxt)
                        ).start()

                    @pl.when(jnp.logical_and(far, row == other) if only_root else far)
                    def _():
                        remote(
                            src, ref_of(other, half, k), zsend.at[kind, 1], second.at[k],
                            (row, other),
                        ).start()

                if only_root:
                    pl.when(jnp.logical_or(far, row == 1))(go)
                else:
                    go()

            k2 = s - begin - SZ * second_depth

            @pl.when(jnp.logical_and(k2 >= 0, k2 < count))
            def _():
                def go():
                    src = ref_of(col, 1 - half, k2)
                    remote(src, src, zsend.at[kind, 1], second.at[k2], (row, col)).wait_recv()

                if only_root:
                    pl.when(mine)(go)
                else:
                    go()

        def a_ref(c, h, k):
            base = jnp.where(row == c, W, 2 * W)
            return rows_of(big, base + h * HB + k * ZR, ZR)

        def l_ref(c, h, k):
            return rows_of(l10, h * (HB // 2) + k * RL, RL)

        def g_ref(c, h, k):
            return rows_of(gbuf, h * HB + k * ZR, ZR)

        def slot(s):
            z_step(s, 0, KZ, a_ref, zr1, zr2, 0, True)
            z_step(s, ZL0, KZL, l_ref, lr1, lr2, 1, False)
            z_step(s, ZG0, KZ, g_ref, gr1, gr2, 2, False)
            for t in range(4):
                k = s - start - SIG * trees[t].depth

                @pl.when(jnp.logical_and(k >= 0, k < 2 * KT))
                def _():
                    tree_step(t, k, (k * 4 + t) * RC, big, RC, tree_send)

        def comm_only(s, _):
            slot(s)
            return 0

        have_l = ZL0 + KZL + 4 * SZ
        lax.fori_loop(0, have_l, comm_only, 0)
        split_inverse()
        split_coupling()
        load_l.wait()

        def with_p(i, _):
            slot(have_l + i)
            p_rows(i * 128, 128, False)
            return 0

        lax.fori_loop(0, 8, with_p, 0)
        begin = 2 * KT + start
        lax.fori_loop(have_l + 8, begin, comm_only, 0)
        load_u.wait()

        def split_l(i, _):
            rows = pl.ds(pl.multiple_of(i * 128, 128), 128)
            h, l = split(big[rows])
            lh[rows] = h
            ll[rows] = l
            return 0

        lax.fori_loop(0, 8, split_l, 0)

        def with_update(v, _):
            slot(begin + v)
            b, w = lax.div(v, 8), lax.rem(v, 8)

            @pl.when(jnp.logical_and(w == 0, b < 4))
            def _():
                h, l = split(big[pl.ds(pl.multiple_of(W + b * 256, 256), 256)])
                ah[0:256] = h
                al[0:256] = l

            @pl.when(jnp.logical_and(w < 4, b < 4))
            def _():
                rows = pl.ds(pl.multiple_of(w * 256, 256), 256)
                cols = pl.ds(pl.multiple_of(b * 256, 256), 256)
                upd = mul3(nt, (ph[rows], plo[rows]), (ah[0:256], al[0:256]))
                u[rows, cols] = u[rows, cols] - jnp.where(top, 0.0, upd)

            @pl.when(jnp.logical_and(w >= 4, b > 0))
            def _():
                h = lax.rem(w, 2)
                c0 = lax.div(w - 4, 2) * HB
                at = h * HB + (b - 1) * 128
                rows = pl.ds(pl.multiple_of(at, 128), 128)
                cols = pl.ds(pl.multiple_of(c0, HB), HB)
                upd = mul3(nt, split(gbuf[rows]), (lh[cols], ll[cols]))
                u[rows, cols] = u[rows, cols] - jnp.where(top, 0.0, upd)
            return 0

        lax.fori_loop(0, 40, with_update, 0)

        for t in range(4):
            for s in range(2):
                @pl.when(trees[t].has[s])
                def _():
                    ref = big.at[pl.ds(0, 2 * KT * RC)]
                    remote(ref, ref, tree_send.at[t, s], lr1.at[0], (row, col)).wait_send()
        for kind in range(3):
            ref = l10.at[pl.ds(0, HB // 2)] if kind == 1 else big.at[pl.ds(0, HB)]

            @pl.when(on)
            def _():
                remote(ref, ref, zsend.at[kind, 0], lr1.at[0], (row, col)).wait_send()

            @pl.when(jnp.logical_and(far, row == other) if kind == 0 else far)
            def _():
                remote(ref, ref, zsend.at[kind, 1], lr1.at[0], (row, col)).wait_send()

    out = pltpu.make_async_copy(u, o_hbm, out_sem)
    out.start()
    out.wait()


def body(a_window, l_panel, l_inverse):
    vmem = pltpu.VMEM
    dma = pltpu.SemaphoreType.DMA
    return pl.pallas_call(
        kernel,
        out_shape=jax.ShapeDtypeStruct((W, W), F32),
        in_specs=[pl.BlockSpec(memory_space=pl.ANY)] * 3,
        out_specs=pl.BlockSpec(memory_space=pl.ANY),
        scratch_shapes=[
            vmem((3 * W, W), F32),
            vmem((W, W), F32),
            vmem((W, W), F32),
            vmem((2, HB, HB), F32),
            vmem((HB, HB), F32),
            vmem((W, W), F32),
            vmem((W, W), BF16), vmem((W, W), BF16),
            vmem((W, W), BF16), vmem((W, W), BF16),
            vmem((W, W), BF16), vmem((W, W), BF16),
            vmem((2, HB, HB), BF16), vmem((2, HB, HB), BF16),
            vmem((HB, HB), BF16), vmem((HB, HB), BF16),
            dma((5,)),
            dma((4, 2 * KT)),
            dma((4, 2)),
            dma((4, 2)),
            dma((KZ,)), dma((KZ,)),
            dma((KZL,)), dma((KZL,)),
            dma((KZ,)), dma((KZ,)),
            dma((3, 4)),
            dma,
        ],
        compiler_params=pltpu.CompilerParams(
            collective_id=0, has_side_effects=True, vmem_limit_bytes=64000000
        ),
        name="block_step",
    )(a_window, l_panel, l_inverse)


def solution(mesh):
    placed = (P("row", "col"), P("row", None), P())
    return jax.shard_map(
        body, mesh=mesh, in_specs=placed, out_specs=P("row", "col"), check_vma=False
    )
```

```python
import jax
import jax.numpy as jnp
from jax import lax
from jax.experimental import pallas as pl
from jax.experimental.pallas import tpu as pltpu
from jax.sharding import PartitionSpec as P

MESH = pl.DeviceIdType.MESH
F32 = jnp.float32
BF16 = jnp.bfloat16

W = 1024
HB = 512
RC = 8
KT = W // (4 * RC)
RP = 16
KP = W // (4 * RP)
RL = 32
KL = HB // (4 * RL)
ZR = 16
KZ = HB // ZR
KZL = HB // 2 // RL
SIG = 6
SP = 5
SZ = 6
SD = 2
ZL0 = 36
ZG0 = 56
DEEP = 6


def split(v):
    hi = v.astype(BF16)
    return hi, (v - hi.astype(F32)).astype(BF16)


def nn(a, b):
    return jnp.dot(a, b, preferred_element_type=F32)


def mul3(a, b):
    return nn(a[0], b[0]) + (nn(a[0], b[1]) + nn(a[1], b[0]))


def wrap(v):
    return lax.rem(v + 4, 4)


class Tree:
    def __init__(self, t, x, y, root):
        rx, ry = lax.rem(root, 4), lax.div(root, 4)
        sgn = 1 if t % 2 == 0 else -1
        dx, dy = wrap((x - rx) * sgn), wrap((y - ry) * sgn)
        main, sec = (dx, dy) if t < 2 else (dy, dx)
        self.depth = jnp.where(main == 0, jnp.where(sec == 0, 0, sec + 2), main + sec)
        self.root = jnp.logical_and(main == 0, sec == 0)
        step = jnp.where(sec == 0, sgn, -sgn)
        self.has = (
            jnp.logical_or(
                jnp.logical_and(sec == 0, main < 3), jnp.logical_and(sec > 0, main == 1)
            ),
            jnp.logical_and(main >= 1, sec < 3),
        )
        if t < 2:
            self.to = (y * 4 + wrap(x + step), wrap(y + sgn) * 4 + x)
        else:
            self.to = (wrap(y + step) * 4 + x, y * 4 + wrap(x + sgn))


def kernel(
    a_hbm, l_hbm, inv_hbm, o_hbm,
    big, u, lr, inv, l10, gbuf, ph, plo, ah, al, lh, ll, ih, il, jh, jl, lth, ltl, mth, mtl,
    load_sem, tree_recv, tree_send, l10_send,
    zr1, zr2, lr1, lr2, gr1, gr2, zsend, out_sem,
):
    row, col = lax.axis_index("row"), lax.axis_index("col")
    x, y = lax.rem(row, 4), lax.div(row, 4)
    z, core = lax.div(col, 2), lax.rem(col, 2)
    other = col + 1 - 2 * core
    top = row == 0

    def remote(src, dst, send, recv, to):
        return pltpu.make_async_remote_copy(
            src_ref=src, dst_ref=dst, send_sem=send, recv_sem=recv,
            device_id=to, device_id_type=MESH,
        )

    def rows_of(ref, at, n):
        return ref.at[pl.ds(pl.multiple_of(at, 8), n)]

    load_inv = pltpu.make_async_copy(inv_hbm, inv, load_sem.at[0])
    load_l = pltpu.make_async_copy(l_hbm, lr, load_sem.at[1])
    load_inv.start()
    load_l.start()

    barrier = pltpu.get_barrier_semaphore()
    peers = [
        (y * 4 + wrap(x + 1), col), (y * 4 + wrap(x - 1), col),
        (wrap(y + 1) * 4 + x, col), (wrap(y - 1) * 4 + x, col),
        (row, other),
        (row, 2 * wrap(z + 1) + core), (row, 2 * wrap(z - 1) + core),
        (row, 2 * wrap(z + jnp.where(core == 0, -1, 1)) + 1 - core),
    ]
    for peer in peers:
        pl.semaphore_signal(barrier, inc=1, device_id=peer, device_id_type=MESH)
    pl.semaphore_wait(barrier, len(peers))

    trees = [Tree(t, x, y, col) for t in range(4)]

    def split_inverse():
        load_inv.wait()
        for b in range(2):
            h, l = split(inv[b])
            ih[b] = h
            il[b] = l

    def split_coupling():
        h, l = split(l10[...])
        lth[...] = h
        ltl[...] = l

    def tree_step(t, k, at, buf, n, send):
        tree = trees[t]
        ref = rows_of(buf, at, n)

        @pl.when(jnp.logical_not(tree.root))
        def _():
            remote(ref, ref, send.at[t, 0], tree_recv.at[t, k], (row, col)).wait_recv()

        for s in range(2):
            @pl.when(tree.has[s])
            def _():
                remote(ref, ref, send.at[t, s], tree_recv.at[t, k], (tree.to[s], col)).start()

    def p_rows(at, n, eye):
        rows = pl.ds(pl.multiple_of(at, 8), n)
        l0, l1 = lr[rows, :HB], lr[rows, HB:]
        if eye:
            i = at + lax.broadcasted_iota(jnp.int32, (n, HB), 0)
            j = lax.broadcasted_iota(jnp.int32, (n, HB), 1)
            l0 = jnp.where(top, jnp.where(i == j, 1.0, 0.0), l0)
            l1 = jnp.where(top, jnp.where(i == j + HB, 1.0, 0.0), l1)
        p1 = split(mul3(split(l1), (ih[1], il[1])))
        ph[rows, HB:] = p1[0]
        plo[rows, HB:] = p1[1]
        p0 = split(
            mul3(split(l0 - mul3(p1, (lth[...], ltl[...]))), (ih[0], il[0]))
        )
        ph[rows, :HB] = p0[0]
        plo[rows, :HB] = p0[1]

    def right_solve(r, put):
        x0 = mul3(split(r[:, :HB]), (jh[0], jl[0]))
        put(0, x0)
        mid = r[:, HB:] - mul3(split(x0), (mth[...], mtl[...]))
        put(HB, mul3(split(mid), (jh[1], jl[1])))

    def out_copy(at, n, i):
        return pltpu.make_async_copy(
            u.at[pl.ds(at, n)], o_hbm.at[pl.ds(at, n)], out_sem.at[i]
        )

    @pl.when(col == 0)
    def _():
        load_a = pltpu.make_async_copy(a_hbm, big.at[pl.ds(2 * W, W)], load_sem.at[2])
        load_a.start()
        load_c = pltpu.make_async_copy(
            l_hbm.at[pl.ds(HB, HB), pl.ds(0, HB)], l10, load_sem.at[3]
        )
        load_t = pltpu.make_async_copy(a_hbm, big.at[pl.ds(0, W)], load_sem.at[4])

        @pl.when(top)
        def _():
            load_c.start()
            load_t.start()
            load_c.wait()
            load_t.wait()

        def send_a(k, _):
            @pl.when(row >= 2)
            def _():
                for half, to in ((0, 2), (1, 7)):
                    src = rows_of(big, 2 * W + half * HB + k * ZR, ZR)
                    at = jnp.where(row == to, W, 2 * W)
                    dst = rows_of(big, at + half * HB + k * ZR, ZR)
                    remote(src, dst, zsend.at[0, half], zr1.at[k], (row, to)).start()

            @pl.when(row == 1)
            def _():
                for half, recv in ((0, zr2), (1, zr1)):
                    src = rows_of(big, 2 * W + half * HB + k * ZR, ZR)
                    dst = rows_of(big, W + half * HB + k * ZR, ZR)
                    remote(src, dst, zsend.at[0, 2 + half], recv.at[k], (row, 1)).start()
            return 0


        def slot(s):
            for t in range(4):
                k = s - SP * trees[t].depth

                @pl.when(jnp.logical_and(k >= 0, k < KL))
                def _():
                    tree_step(t, k, (k * 4 + t) * RL, l10, RL, l10_send)

                k2 = k - KL

                @pl.when(jnp.logical_and(k2 >= 0, k2 < KP))
                def _():
                    tree_step(t, k2 + KL, (k2 * 4 + t) * RP, big, RP, tree_send)

        first = KL + SP * DEEP

        def comm_only(s, _):
            slot(s)
            return 0

        lax.fori_loop(0, 2, comm_only, 0)
        load_a.wait()

        def with_send(i, _):
            slot(2 + i)

            @pl.when(jnp.logical_and(row >= 1, row < 8))
            def _():
                lax.fori_loop(4 * i, 4 * i + 4, send_a, 0)
            return 0

        lax.fori_loop(0, KZ // 4, with_send, 0)
        split_inverse()
        lax.fori_loop(10, 12, comm_only, 0)
        for b in range(2):
            h, l = split(inv[b].T)
            jh[b] = h
            jl[b] = l
        load_l.wait()
        lax.fori_loop(12, first, comm_only, 0)

        def send_l(k, _):
            for half, to in ((0, 2), (1, 7)):
                ref = rows_of(l10, half * (HB // 2) + k * RL, RL)
                remote(ref, ref, zsend.at[1, half], lr1.at[k], (row, to)).start()
            for half, recv in ((0, lr2), (1, lr1)):
                ref = rows_of(l10, half * (HB // 2) + k * RL, RL)
                remote(ref, ref, zsend.at[1, 2 + half], recv.at[k], (row, 1)).start()
            return 0

        lax.fori_loop(0, KZL, send_l, 0)
        split_coupling()
        h, l = split(l10[...].T)
        mth[...] = h
        mtl[...] = l

        def with_p(i, _):
            slot(first + 2 * i)
            slot(first + 2 * i + 1)
            p_rows(i * 256, 256, True)
            return 0

        lax.fori_loop(0, 4, with_p, 0)
        lax.fori_loop(first + 8, KL + KP + SP * DEEP, comm_only, 0)

        def split_t(i, _):
            rows = pl.ds(pl.multiple_of(i * 128, 128), 128)
            h, l = split(big[pl.ds(pl.multiple_of(i * 128, 128), 128)] + big[0:W, rows].T)
            lh[rows] = h
            ll[rows] = l
            return 0

        lax.fori_loop(0, 8, split_t, 0)

        def place(g):
            half, q = lax.rem(g, 2), lax.div(g, 2)
            return half, q, half * HB + q * 128

        def send_block(g):
            half, q, at = place(g)

            def send_g(j, _):
                ref = rows_of(gbuf, at + j * ZR, ZR)
                k = q * (128 // ZR) + j

                @pl.when(half == 0)
                def _():
                    remote(ref, ref, zsend.at[2, 0], gr1.at[k], (row, 2)).start()
                    remote(ref, ref, zsend.at[2, 2], gr2.at[k], (row, 1)).start()

                @pl.when(half == 1)
                def _():
                    remote(ref, ref, zsend.at[2, 1], gr1.at[k], (row, 7)).start()
                    remote(ref, ref, zsend.at[2, 3], gr1.at[k], (row, 1)).start()
                return 0

            lax.fori_loop(0, 128 // ZR, send_g, 0)

        def g_block(g, _):
            _, _, at = place(g)
            rows = pl.ds(pl.multiple_of(at, 128), 128)
            p = (ph[rows], plo[rows])

            def part(n):
                cols = slice(n * HB, n * HB + HB)
                pt = mul3(p, (lh[:, cols], ll[:, cols]))
                a = big[pl.ds(pl.multiple_of(2 * W + at, 128), 128), cols]
                gbuf[rows, cols] = a - 0.5 * pt

            part(0)

            @pl.when(g > 0)
            def _():
                send_block(g - 1)

            part(1)

            def put_g(c0, v):
                gbuf[rows, c0:c0 + HB] = v

            right_solve(gbuf[rows], put_g)
            return 0

        lax.fori_loop(0, 8, g_block, 0)

        def split_a(i, _):
            rows = pl.ds(pl.multiple_of(i * 128, 128), 128)
            h, l = split(big[rows])
            ah[rows] = h
            al[rows] = l
            return 0

        lax.fori_loop(0, 8, split_a, 0)
        send_block(7)

        def o_block(g, _):
            rows = pl.ds(pl.multiple_of(g * 128, 128), 128)
            p = (ph[rows], plo[rows])
            for n in range(2):
                cols = slice(n * HB, n * HB + HB)
                e = mul3(p, (ah[:, cols], al[:, cols]))
                a = big[pl.ds(pl.multiple_of(2 * W + g * 128, 128), 128), cols]
                u[rows, cols] = jnp.where(top, e, a - e)

            def put_o(c0, v):
                u[rows, c0:c0 + HB] = v

            right_solve(u[rows], put_o)
            return 0

        lax.fori_loop(0, 4, o_block, 0)
        early = out_copy(0, HB, 0)
        early.start()
        lax.fori_loop(4, 8, o_block, 0)
        late = out_copy(HB, HB, 1)
        late.start()
        early.wait()
        late.wait()

        for t in range(4):
            for s in range(2):
                @pl.when(trees[t].has[s])
                def _():
                    ref = l10.at[pl.ds(0, KL * RL)]
                    remote(ref, ref, l10_send.at[t, s], lr1.at[0], (row, 1)).wait_send()
                    ref = big.at[pl.ds(0, KP * RP)]
                    remote(ref, ref, tree_send.at[t, s], lr1.at[0], (row, 1)).wait_send()
        for s in range(4):
            ref = big.at[pl.ds(0, HB)]
            @pl.when(jnp.logical_and(row >= 2, row < 8) if s < 2 else row == 1)
            def _():
                remote(ref, ref, zsend.at[0, s], lr1.at[0], (row, 1)).wait_send()

            remote(ref, ref, zsend.at[2, s], lr1.at[0], (row, 1)).wait_send()
            ref = l10.at[pl.ds(0, HB // 2)]
            remote(ref, ref, zsend.at[1, s], lr1.at[0], (row, 1)).wait_send()

    @pl.when(col > 0)
    def _():
        load_u = pltpu.make_async_copy(a_hbm, u, load_sem.at[2])
        load_u.start()
        mine = row == col
        load_r = pltpu.make_async_copy(l_hbm, big.at[pl.ds(0, W)], load_sem.at[4])

        @pl.when(mine)
        def _():
            load_r.start()
            load_r.wait()

        far = z > 0
        zrow = jnp.logical_and(far, jnp.logical_and(row >= 2, row < 8))
        first_slots = jnp.where(far, SZ * jnp.where(core == 0, z, 4 - z), SD)
        second_slots = jnp.where(far, SZ * jnp.where(core == 0, 4 - z, z) + SD, SD)
        on = jnp.where(core == 0, jnp.logical_and(far, z < 3), z > 1)
        nxt = jnp.where(core == 0, col + 2, col - 2)
        half = jnp.where(core == 0, 0, 1)

        def z_step(s, begin, count, ref_of, first, second, kind, only_root):
            k = s - begin - first_slots

            @pl.when(jnp.logical_and(k >= 0, k < count))
            def _():
                def go():
                    src = ref_of(col, half, k)
                    remote(src, src, zsend.at[kind, 0], first.at[k], (row, col)).wait_recv()

                    @pl.when(on)
                    def _():
                        remote(
                            src, ref_of(nxt, half, k), zsend.at[kind, 0], first.at[k], (row, nxt)
                        ).start()

                    @pl.when(jnp.logical_and(far, row == other) if only_root else far)
                    def _():
                        remote(
                            src, ref_of(other, half, k), zsend.at[kind, 1], second.at[k],
                            (row, other),
                        ).start()

                if only_root:
                    pl.when(zrow)(go)
                else:
                    go()

            k2 = s - begin - second_slots

            @pl.when(jnp.logical_and(k2 >= 0, k2 < count))
            def _():
                def go():
                    src = ref_of(col, 1 - half, k2)
                    remote(src, src, zsend.at[kind, 1], second.at[k2], (row, col)).wait_recv()

                if only_root:
                    pl.when(jnp.logical_and(zrow, mine))(go)
                else:
                    go()

        def a_ref(c, h, k):
            base = jnp.where(row == c, W, 2 * W)
            return rows_of(big, base + h * HB + k * ZR, ZR)

        def l_ref(c, h, k):
            return rows_of(l10, h * (HB // 2) + k * RL, RL)

        def g_ref(c, h, k):
            return rows_of(gbuf, h * HB + k * ZR, ZR)

        @pl.when(jnp.logical_and(mine, col == 1))
        def _():
            def arrive(k, _):
                ref = rows_of(big, W + k * ZR, ZR)
                remote(ref, ref, zsend.at[0, 0], zr1.at[k], (row, col)).wait_recv()
                remote(ref, ref, zsend.at[0, 0], zr2.at[k], (row, col)).wait_recv()
                return 0

            lax.fori_loop(0, KZ, arrive, 0)

        def slot(s):
            z_step(s, 0, KZ, a_ref, zr1, zr2, 0, True)
            z_step(s, ZL0, KZL, l_ref, lr1, lr2, 1, False)
            z_step(s, ZG0, KZ, g_ref, gr1, gr2, 2, False)
            for t in range(4):
                k = s - SIG * trees[t].depth

                @pl.when(jnp.logical_and(k >= 0, k < 2 * KT))
                def _():
                    m, i = lax.div(k, KT), lax.rem(k, KT)
                    at = m * W + (t // 2) * HB + i * 2 * RC + (t % 2) * RC
                    tree_step(t, k, at, big, RC, tree_send)

        def comm_only(s, _):
            slot(s)
            return 0

        have_l = ZL0 + KZL + 3 * SZ + SD
        lax.fori_loop(0, 20, comm_only, 0)
        split_inverse()
        lax.fori_loop(20, have_l, comm_only, 0)
        split_coupling()
        load_l.wait()

        def with_p(i, _):
            slot(have_l + 2 * i)
            slot(have_l + 2 * i + 1)
            p_rows(i * 256, 256, False)
            return 0

        lax.fori_loop(0, 4, with_p, 0)
        begin = KT + 8 + SIG * DEEP
        assert begin == have_l + 12
        load_u.wait()

        def split_l(i, _):
            slot(have_l + 8 + i)
            for j in range(2):
                at = i * 256 + j * 128
                cols = pl.ds(pl.multiple_of(at, 128), 128)
                h, l = split(big[pl.ds(pl.multiple_of(at, 128), 128)].T)
                lh[:, cols] = h
                ll[:, cols] = l
            return 0

        lax.fori_loop(0, 4, split_l, 0)

        def with_update(v, _):
            slot(begin + v)
            b, w = lax.div(v, 8), lax.rem(v, 8)

            @pl.when(jnp.logical_and(w == 0, b < 4))
            def _():
                for j in range(2):
                    at = W + j * HB + b * 128
                    h, l = split(big[pl.ds(pl.multiple_of(at, 128), 128)].T)
                    ah[:, j * 128:j * 128 + 128] = h
                    al[:, j * 128:j * 128 + 128] = l

            @pl.when(jnp.logical_and(jnp.logical_or(w == 1, w == 3), b < 4))
            def _():
                rows = pl.ds(pl.multiple_of(lax.div(w, 2) * HB, HB), HB)
                upd = mul3((ph[rows], plo[rows]), (ah[:, 0:256], al[:, 0:256]))
                for j in range(2):
                    cols = pl.ds(pl.multiple_of(j * HB + b * 128, 128), 128)
                    part = jnp.where(top, 0.0, upd[:, j * 128:j * 128 + 128])
                    u[rows, cols] = u[rows, cols] - part

            @pl.when(jnp.logical_and(jnp.logical_or(w == 5, w == 7), b > 0))
            def _():
                at = lax.div(w - 5, 2) * HB + (b - 1) * 128
                rows = pl.ds(pl.multiple_of(at, 128), 128)
                g = split(gbuf[rows])
                for j in range(2):
                    cols = slice(j * HB, j * HB + HB)
                    upd = mul3(g, (lh[:, cols], ll[:, cols]))
                    u[rows, cols] = u[rows, cols] - jnp.where(top, 0.0, upd)
            return 0

        lax.fori_loop(0, 32, with_update, 0)
        early = [out_copy(h * HB, 384, h) for h in range(2)]
        for c in early:
            c.start()
        lax.fori_loop(32, 40, with_update, 0)
        late = [out_copy(h * HB + 384, 128, 2 + h) for h in range(2)]
        for c in late:
            c.start()
        for c in early + late:
            c.wait()

        for t in range(4):
            for s in range(2):
                @pl.when(trees[t].has[s])
                def _():
                    ref = big.at[pl.ds(0, 2 * KT * RC)]
                    remote(ref, ref, tree_send.at[t, s], lr1.at[0], (row, col)).wait_send()
        for kind in range(3):
            ref = l10.at[pl.ds(0, HB // 2)] if kind == 1 else big.at[pl.ds(0, HB)]

            @pl.when(jnp.logical_and(zrow, on) if kind == 0 else on)
            def _():
                remote(ref, ref, zsend.at[kind, 0], lr1.at[0], (row, col)).wait_send()

            @pl.when(jnp.logical_and(zrow, row == other) if kind == 0 else far)
            def _():
                remote(ref, ref, zsend.at[kind, 1], lr1.at[0], (row, col)).wait_send()


def body(a_window, l_panel, l_inverse):
    vmem = pltpu.VMEM
    dma = pltpu.SemaphoreType.DMA
    return pl.pallas_call(
        kernel,
        out_shape=jax.ShapeDtypeStruct((W, W), F32),
        in_specs=[pl.BlockSpec(memory_space=pl.ANY)] * 3,
        out_specs=pl.BlockSpec(memory_space=pl.ANY),
        scratch_shapes=[
            vmem((3 * W, W), F32),
            vmem((W, W), F32),
            vmem((W, W), F32),
            vmem((2, HB, HB), F32),
            vmem((HB, HB), F32),
            vmem((W, W), F32),
            vmem((W, W), BF16), vmem((W, W), BF16),
            vmem((W, W), BF16), vmem((W, W), BF16),
            vmem((W, W), BF16), vmem((W, W), BF16),
            vmem((2, HB, HB), BF16), vmem((2, HB, HB), BF16),
            vmem((2, HB, HB), BF16), vmem((2, HB, HB), BF16),
            vmem((HB, HB), BF16), vmem((HB, HB), BF16),
            vmem((HB, HB), BF16), vmem((HB, HB), BF16),
            dma((5,)),
            dma((4, 2 * KT)),
            dma((4, 2)),
            dma((4, 2)),
            dma((KZ,)), dma((KZ,)),
            dma((KZL,)), dma((KZL,)),
            dma((KZ,)), dma((KZ,)),
            dma((3, 4)),
            dma((4,)),
        ],
        compiler_params=pltpu.CompilerParams(
            collective_id=0, has_side_effects=True, vmem_limit_bytes=64000000
        ),
        name="block_step",
    )(a_window, l_panel, l_inverse)


def solution(mesh):
    placed = (P("row", "col"), P("row", None), P())
    return jax.shard_map(
        body, mesh=mesh, in_specs=placed, out_specs=P("row", "col"), check_vma=False
    )
```

```python
import jax
import jax.numpy as jnp
from jax import lax
from jax.experimental import pallas as pl
from jax.experimental.pallas import tpu as pltpu
from jax.sharding import PartitionSpec as P

MESH = pl.DeviceIdType.MESH
F32 = jnp.float32
BF16 = jnp.bfloat16

W = 1024
HB = 512
RC = 8
KT = W // (4 * RC)
RP = 8
KP = W // (4 * RP)
RL = 16
KL = HB // (4 * RL)
ZR = 16
KZ = HB // ZR
RZ = 32
KZL = HB // 2 // RZ
SIG = 6
SP = 9
SZ = 6
SD = 2
ZL0 = 36
ZG0 = 62
DEEP = 6
HOLD = 56


def split(v):
    hi = v.astype(BF16)
    return hi, (v - hi.astype(F32)).astype(BF16)


def nn(a, b):
    return jnp.dot(a, b, preferred_element_type=F32)


def mul3(a, b):
    return nn(a[0], b[0]) + (nn(a[0], b[1]) + nn(a[1], b[0]))


def wrap(v):
    return lax.rem(v + 4, 4)


class Tree:
    def __init__(self, t, x, y, root):
        rx, ry = lax.rem(root, 4), lax.div(root, 4)
        sgn = 1 if t % 2 == 0 else -1
        dx, dy = wrap((x - rx) * sgn), wrap((y - ry) * sgn)
        main, sec = (dx, dy) if t < 2 else (dy, dx)
        self.depth = jnp.where(main == 0, jnp.where(sec == 0, 0, sec + 2), main + sec)
        self.root = jnp.logical_and(main == 0, sec == 0)
        step = jnp.where(sec == 0, sgn, -sgn)
        self.has = (
            jnp.logical_or(
                jnp.logical_and(sec == 0, main < 3), jnp.logical_and(sec > 0, main == 1)
            ),
            jnp.logical_and(main >= 1, sec < 3),
        )
        if t < 2:
            self.to = (y * 4 + wrap(x + step), wrap(y + sgn) * 4 + x)
        else:
            self.to = (wrap(y + step) * 4 + x, y * 4 + wrap(x + sgn))


def kernel(
    a_hbm, l_hbm, inv, u,
    big, lr, l10, gbuf, ph, plo, ah, al, lh, ll, ih, il, jh, jl, lth, ltl, mth, mtl,
    load_sem, tree_recv, tree_send, l10_send,
    zr1, zr2, lr1, lr2, gr1, gr2, zsend,
):
    row, col = lax.axis_index("row"), lax.axis_index("col")
    x, y = lax.rem(row, 4), lax.div(row, 4)
    z, core = lax.div(col, 2), lax.rem(col, 2)
    other = col + 1 - 2 * core
    top = row == 0

    def remote(src, dst, send, recv, to):
        return pltpu.make_async_remote_copy(
            src_ref=src, dst_ref=dst, send_sem=send, recv_sem=recv,
            device_id=to, device_id_type=MESH,
        )

    def rows_of(ref, at, n):
        return ref.at[pl.ds(pl.multiple_of(at, 8), n)]

    load_l = pltpu.make_async_copy(l_hbm, lr, load_sem.at[1])
    load_a = pltpu.make_async_copy(a_hbm, big.at[pl.ds(2 * W, W)], load_sem.at[2])
    load_u = pltpu.make_async_copy(a_hbm, u, load_sem.at[2])
    load_c = pltpu.make_async_copy(
        l_hbm.at[pl.ds(HB, HB), pl.ds(0, HB)], l10, load_sem.at[3]
    )
    load_t = pltpu.make_async_copy(a_hbm, big.at[pl.ds(0, W)], load_sem.at[4])
    load_r = pltpu.make_async_copy(l_hbm, big.at[pl.ds(0, W)], load_sem.at[4])
    panel = col == 0
    mine = row == col

    @pl.when(jnp.logical_and(mine, panel))
    def _():
        load_c.start()
        load_t.start()

    @pl.when(jnp.logical_and(mine, jnp.logical_not(panel)))
    def _():
        load_r.start()

    @pl.when(panel)
    def _():
        load_a.start()

    @pl.when(jnp.logical_not(panel))
    def _():
        load_u.start()

    load_l.start()

    barrier = pltpu.get_barrier_semaphore()
    peers = [
        (y * 4 + wrap(x + 1), col), (y * 4 + wrap(x - 1), col),
        (wrap(y + 1) * 4 + x, col), (wrap(y - 1) * 4 + x, col),
        (row, other),
        (row, 2 * wrap(z + 1) + core), (row, 2 * wrap(z - 1) + core),
        (row, 2 * wrap(z + jnp.where(core == 0, -1, 1)) + 1 - core),
    ]
    for peer in peers:
        pl.semaphore_signal(barrier, inc=1, device_id=peer, device_id_type=MESH)
    pl.semaphore_wait(barrier, len(peers))

    trees = [Tree(t, x, y, col) for t in range(4)]

    def split_inverse():
        for b in range(2):
            h, l = split(inv[b])
            ih[b] = h
            il[b] = l

    def split_coupling():
        h, l = split(l10[...])
        lth[...] = h
        ltl[...] = l

    def tree_step(t, k, at, buf, n, send):
        tree = trees[t]
        ref = rows_of(buf, at, n)

        @pl.when(jnp.logical_not(tree.root))
        def _():
            remote(ref, ref, send.at[t, 0], tree_recv.at[t, k], (row, col)).wait_recv()

        for s in range(2):
            @pl.when(tree.has[s])
            def _():
                remote(ref, ref, send.at[t, s], tree_recv.at[t, k], (tree.to[s], col)).start()

    def p_rows(at, n, eye):
        rows = pl.ds(pl.multiple_of(at, 8), n)
        l0, l1 = lr[rows, :HB], lr[rows, HB:]
        if eye:
            i = at + lax.broadcasted_iota(jnp.int32, (n, HB), 0)
            j = lax.broadcasted_iota(jnp.int32, (n, HB), 1)
            l0 = jnp.where(top, jnp.where(i == j, 1.0, 0.0), l0)
            l1 = jnp.where(top, jnp.where(i == j + HB, 1.0, 0.0), l1)
        p1 = split(mul3(split(l1), (ih[1], il[1])))
        ph[rows, HB:] = p1[0]
        plo[rows, HB:] = p1[1]
        p0 = split(
            mul3(split(l0 - mul3(p1, (lth[...], ltl[...]))), (ih[0], il[0]))
        )
        ph[rows, :HB] = p0[0]
        plo[rows, :HB] = p0[1]

    def right_solve(r, put):
        x0 = mul3(split(r[:, :HB]), (jh[0], jl[0]))
        put(0, x0)
        mid = r[:, HB:] - mul3(split(x0), (mth[...], mtl[...]))
        put(HB, mul3(split(mid), (jh[1], jl[1])))

    @pl.when(col == 0)
    def _():
        @pl.when(top)
        def _():
            load_c.wait()
            load_t.wait()

        def send_a(k, _):
            @pl.when(row >= 2)
            def _():
                for half, to in ((0, 2), (1, 7)):
                    src = rows_of(big, 2 * W + half * HB + k * ZR, ZR)
                    at = jnp.where(row == to, W, 2 * W)
                    dst = rows_of(big, at + half * HB + k * ZR, ZR)
                    remote(src, dst, zsend.at[0, half], zr1.at[k], (row, to)).start()

            @pl.when(row == 1)
            def _():
                for half, recv in ((0, zr2), (1, zr1)):
                    src = rows_of(big, 2 * W + half * HB + k * ZR, ZR)
                    dst = rows_of(big, W + half * HB + k * ZR, ZR)
                    remote(src, dst, zsend.at[0, 2 + half], recv.at[k], (row, 1)).start()
            return 0


        def slot(s):
            for t in range(4):
                k = s - SP * trees[t].depth

                @pl.when(jnp.logical_and(k >= 0, k < KL))
                def _():
                    tree_step(t, k, (k * 4 + t) * RL, l10, RL, l10_send)

                k2 = k - KL

                @pl.when(jnp.logical_and(k2 >= 0, k2 < KP))
                def _():
                    tree_step(t, k2 + KL, (k2 * 4 + t) * RP, big, RP, tree_send)

        first = KL + SP * DEEP

        def comm_only(s, _):
            slot(s)
            return 0

        lax.fori_loop(0, 4, comm_only, 0)
        load_a.wait()

        def with_send(i, _):
            slot(4 + i)

            @pl.when(jnp.logical_and(row >= 2, row < 8))
            def _():
                lax.fori_loop(2 * i, 2 * i + 2, send_a, 0)
            return 0

        lax.fori_loop(0, KZ // 2, with_send, 0)
        split_inverse()
        lax.fori_loop(20, 24, comm_only, 0)
        for b in range(2):
            h, l = split(inv[b].T)
            jh[b] = h
            jl[b] = l
        load_l.wait()
        lax.fori_loop(24, HOLD, comm_only, 0)

        @pl.when(row == 1)
        def _():
            lax.fori_loop(0, KZ, send_a, 0)

        lax.fori_loop(HOLD, first, comm_only, 0)

        def send_l(k, _):
            for half, to in ((0, 2), (1, 7)):
                ref = rows_of(l10, half * (HB // 2) + k * RZ, RZ)
                remote(ref, ref, zsend.at[1, half], lr1.at[k], (row, to)).start()
            for half, recv in ((0, lr2), (1, lr1)):
                ref = rows_of(l10, half * (HB // 2) + k * RZ, RZ)
                remote(ref, ref, zsend.at[1, 2 + half], recv.at[k], (row, 1)).start()
            return 0

        lax.fori_loop(0, KZL, send_l, 0)
        split_coupling()
        h, l = split(l10[...].T)
        mth[...] = h
        mtl[...] = l

        def with_p(i, _):
            for j in range(4):
                slot(first + 4 * i + j)
            p_rows(i * 128, 128, True)
            return 0

        lax.fori_loop(0, 8, with_p, 0)
        lax.fori_loop(first + 32, KL + KP + SP * DEEP, comm_only, 0)

        def split_t(i, _):
            rows = pl.ds(pl.multiple_of(i * 128, 128), 128)
            h, l = split(big[pl.ds(pl.multiple_of(i * 128, 128), 128)] + big[0:W, rows].T)
            lh[rows] = h
            ll[rows] = l
            return 0

        lax.fori_loop(0, 8, split_t, 0)

        def place(g):
            half, q = lax.rem(g, 2), lax.div(g, 2)
            return half, q, half * HB + q * 128

        def send_block(g):
            half, q, at = place(g)

            def send_g(j, _):
                ref = rows_of(gbuf, at + j * ZR, ZR)
                k = q * (128 // ZR) + j

                @pl.when(half == 0)
                def _():
                    remote(ref, ref, zsend.at[2, 0], gr1.at[k], (row, 2)).start()
                    remote(ref, ref, zsend.at[2, 2], gr2.at[k], (row, 1)).start()

                @pl.when(half == 1)
                def _():
                    remote(ref, ref, zsend.at[2, 1], gr1.at[k], (row, 7)).start()
                    remote(ref, ref, zsend.at[2, 3], gr1.at[k], (row, 1)).start()
                return 0

            lax.fori_loop(0, 128 // ZR, send_g, 0)

        def g_block(g, _):
            _, _, at = place(g)
            rows = pl.ds(pl.multiple_of(at, 128), 128)
            p = (ph[rows], plo[rows])

            def part(n):
                cols = slice(n * HB, n * HB + HB)
                pt = mul3(p, (lh[:, cols], ll[:, cols]))
                a = big[pl.ds(pl.multiple_of(2 * W + at, 128), 128), cols]
                gbuf[rows, cols] = a - 0.5 * pt

            part(0)

            @pl.when(g > 0)
            def _():
                send_block(g - 1)

            part(1)

            def put_g(c0, v):
                gbuf[rows, c0:c0 + HB] = v

            right_solve(gbuf[rows], put_g)
            return 0

        lax.fori_loop(0, 8, g_block, 0)

        def split_a(i, _):
            rows = pl.ds(pl.multiple_of(i * 128, 128), 128)
            h, l = split(big[rows])
            ah[rows] = h
            al[rows] = l
            return 0

        lax.fori_loop(0, 8, split_a, 0)
        send_block(7)

        def o_block(g, _):
            rows = pl.ds(pl.multiple_of(g * 128, 128), 128)
            p = (ph[rows], plo[rows])
            for n in range(2):
                cols = slice(n * HB, n * HB + HB)
                e = mul3(p, (ah[:, cols], al[:, cols]))
                a = big[pl.ds(pl.multiple_of(2 * W + g * 128, 128), 128), cols]
                u[rows, cols] = jnp.where(top, e, a - e)

            def put_o(c0, v):
                u[rows, c0:c0 + HB] = v

            right_solve(u[rows], put_o)
            return 0

        lax.fori_loop(0, 4, o_block, 0)
        lax.fori_loop(4, 8, o_block, 0)
        for t in range(4):
            for s in range(2):
                @pl.when(trees[t].has[s])
                def _():
                    ref = l10.at[pl.ds(0, KL * RL)]
                    remote(ref, ref, l10_send.at[t, s], lr1.at[0], (row, 1)).wait_send()
                    ref = big.at[pl.ds(0, KP * RP)]
                    remote(ref, ref, tree_send.at[t, s], lr1.at[0], (row, 1)).wait_send()
        for s in range(4):
            ref = big.at[pl.ds(0, HB)]
            @pl.when(jnp.logical_and(row >= 2, row < 8) if s < 2 else row == 1)
            def _():
                remote(ref, ref, zsend.at[0, s], lr1.at[0], (row, 1)).wait_send()

            remote(ref, ref, zsend.at[2, s], lr1.at[0], (row, 1)).wait_send()
            ref = l10.at[pl.ds(0, HB // 2)]
            remote(ref, ref, zsend.at[1, s], lr1.at[0], (row, 1)).wait_send()

    def trailing(one):
        rc, sig = (16, 5) if one else (RC, SIG)
        kt = W // (4 * rc)
        zl0, zg0 = (4, 30) if one else (ZL0, ZG0)
        have_l = zl0 + KZL + (SD if one else 3 * SZ + SD)
        begin = kt + kt // 4 + sig * DEEP
        lag = 0 if one else 1
        per = kt // 4
        a_at, g_at = ((0, 1), (2, 3)) if one else ((1, 3), (5, 7))

        @pl.when(mine)
        def _():
            load_r.wait()

        far = z > 0
        zrow = jnp.logical_and(far, jnp.logical_and(row >= 2, row < 8))
        first_slots = jnp.where(far, SZ * jnp.where(core == 0, z, 4 - z), SD)
        second_slots = jnp.where(far, SZ * jnp.where(core == 0, 4 - z, z) + SD, SD)
        on = jnp.where(core == 0, jnp.logical_and(far, z < 3), z > 1)
        nxt = jnp.where(core == 0, col + 2, col - 2)
        half = jnp.where(core == 0, 0, 1)

        def z_step(s, begin, count, ref_of, first, second, kind, only_root):
            k = s - begin - first_slots

            @pl.when(jnp.logical_and(k >= 0, k < count))
            def _():
                def go():
                    src = ref_of(col, half, k)
                    remote(src, src, zsend.at[kind, 0], first.at[k], (row, col)).wait_recv()

                    @pl.when(on)
                    def _():
                        remote(
                            src, ref_of(nxt, half, k), zsend.at[kind, 0], first.at[k], (row, nxt)
                        ).start()

                    @pl.when(jnp.logical_and(far, row == other) if only_root else far)
                    def _():
                        remote(
                            src, ref_of(other, half, k), zsend.at[kind, 1], second.at[k],
                            (row, other),
                        ).start()

                if only_root:
                    pl.when(zrow)(go)
                else:
                    go()

            k2 = s - begin - second_slots

            @pl.when(jnp.logical_and(k2 >= 0, k2 < count))
            def _():
                def go():
                    src = ref_of(col, 1 - half, k2)
                    remote(src, src, zsend.at[kind, 1], second.at[k2], (row, col)).wait_recv()

                if only_root:
                    pl.when(jnp.logical_and(zrow, mine))(go)
                else:
                    go()

        def a_ref(c, h, k):
            base = jnp.where(row == c, W, 2 * W)
            return rows_of(big, base + h * HB + k * ZR, ZR)

        def l_ref(c, h, k):
            return rows_of(l10, h * (HB // 2) + k * RZ, RZ)

        def g_ref(c, h, k):
            return rows_of(gbuf, h * HB + k * ZR, ZR)

        if one:
            @pl.when(mine)
            def _():
                def arrive(k, _):
                    ref = rows_of(big, W + k * ZR, ZR)
                    remote(ref, ref, zsend.at[0, 0], zr1.at[k], (row, col)).wait_recv()
                    remote(ref, ref, zsend.at[0, 0], zr2.at[k], (row, col)).wait_recv()
                    return 0

                lax.fori_loop(0, KZ, arrive, 0)

        def slot(s):
            if not one:
                z_step(s, 0, KZ, a_ref, zr1, zr2, 0, True)
            z_step(s, zl0, KZL, l_ref, lr1, lr2, 1, False)
            z_step(s, zg0, KZ, g_ref, gr1, gr2, 2, False)
            for t in range(4):
                k = s - sig * trees[t].depth

                @pl.when(jnp.logical_and(k >= 0, k < 2 * kt))
                def _():
                    m, i = lax.div(k, kt), lax.rem(k, kt)
                    at = m * W + (t // 2) * HB + i * 2 * rc + (t % 2) * rc
                    tree_step(t, k, at, big, rc, tree_send)

        def comm_only(s, _):
            slot(s)
            return 0

        early = min(20, have_l)
        lax.fori_loop(0, early, comm_only, 0)
        split_inverse()
        lax.fori_loop(early, have_l, comm_only, 0)
        split_coupling()
        load_l.wait()

        def with_p(i, _):
            slot(have_l + 2 * i)
            slot(have_l + 2 * i + 1)
            p_rows(i * 256, 256, False)
            return 0

        lax.fori_loop(0, 4, with_p, 0)
        assert have_l + 12 <= begin
        lax.fori_loop(have_l + 8, begin - 4, comm_only, 0)
        load_u.wait()

        def split_l(i, _):
            slot(begin - 4 + i)
            for j in range(2):
                at = i * 256 + j * 128
                cols = pl.ds(pl.multiple_of(at, 128), 128)
                h, l = split(big[pl.ds(pl.multiple_of(at, 128), 128)].T)
                lh[:, cols] = h
                ll[:, cols] = l
            return 0

        lax.fori_loop(0, 4, split_l, 0)

        def with_update(v, _):
            slot(begin + v)
            b, w = lax.div(v, per), lax.rem(v, per)

            @pl.when(jnp.logical_and(w == 0, b < 4))
            def _():
                for j in range(2):
                    at = W + j * HB + b * 128
                    h, l = split(big[pl.ds(pl.multiple_of(at, 128), 128)].T)
                    ah[:, j * 128:j * 128 + 128] = h
                    al[:, j * 128:j * 128 + 128] = l

            @pl.when(jnp.logical_and(jnp.logical_or(w == a_at[0], w == a_at[1]), b < 4))
            def _():
                rows = pl.ds(pl.multiple_of(jnp.where(w == a_at[1], HB, 0), HB), HB)
                upd = mul3((ph[rows], plo[rows]), (ah[:, 0:256], al[:, 0:256]))
                for j in range(2):
                    cols = pl.ds(pl.multiple_of(j * HB + b * 128, 128), 128)
                    part = jnp.where(top, 0.0, upd[:, j * 128:j * 128 + 128])
                    u[rows, cols] = u[rows, cols] - part

            gb = b - lag

            @pl.when(jnp.logical_and(jnp.logical_or(w == g_at[0], w == g_at[1]), gb >= 0))
            def _():
                at = jnp.where(w == g_at[1], HB, 0) + gb * 128
                rows = pl.ds(pl.multiple_of(at, 128), 128)
                g = split(gbuf[rows])
                for j in range(2):
                    cols = slice(j * HB, j * HB + HB)
                    upd = mul3(g, (lh[:, cols], ll[:, cols]))
                    u[rows, cols] = u[rows, cols] - jnp.where(top, 0.0, upd)
            return 0

        lax.fori_loop(0, per * (4 + lag), with_update, 0)
        for t in range(4):
            for s in range(2):
                @pl.when(trees[t].has[s])
                def _():
                    ref = big.at[pl.ds(0, HB)]
                    remote(ref, ref, tree_send.at[t, s], lr1.at[0], (row, col)).wait_send()
        for kind in range(3):
            ref = l10.at[pl.ds(0, HB // 2)] if kind == 1 else big.at[pl.ds(0, HB)]

            @pl.when(jnp.logical_and(zrow, on) if kind == 0 else on)
            def _():
                remote(ref, ref, zsend.at[kind, 0], lr1.at[0], (row, col)).wait_send()

            @pl.when(jnp.logical_and(zrow, row == other) if kind == 0 else far)
            def _():
                remote(ref, ref, zsend.at[kind, 1], lr1.at[0], (row, col)).wait_send()


    @pl.when(col == 1)
    def _():
        trailing(True)

    @pl.when(col > 1)
    def _():
        trailing(False)


def body(a_window, l_panel, l_inverse):
    vmem = pltpu.VMEM
    dma = pltpu.SemaphoreType.DMA
    return pl.pallas_call(
        kernel,
        out_shape=jax.ShapeDtypeStruct((W, W), F32),
        in_specs=[pl.BlockSpec(memory_space=pl.ANY)] * 2 + [pl.BlockSpec(memory_space=pltpu.VMEM)],
        out_specs=pl.BlockSpec(memory_space=pltpu.VMEM),
        scratch_shapes=[
            vmem((3 * W, W), F32),
            vmem((W, W), F32),
            vmem((HB, HB), F32),
            vmem((W, W), F32),
            vmem((W, W), BF16), vmem((W, W), BF16),
            vmem((W, W), BF16), vmem((W, W), BF16),
            vmem((W, W), BF16), vmem((W, W), BF16),
            vmem((2, HB, HB), BF16), vmem((2, HB, HB), BF16),
            vmem((2, HB, HB), BF16), vmem((2, HB, HB), BF16),
            vmem((HB, HB), BF16), vmem((HB, HB), BF16),
            vmem((HB, HB), BF16), vmem((HB, HB), BF16),
            dma((5,)),
            dma((4, 2 * KT)),
            dma((4, 2)),
            dma((4, 2)),
            dma((KZ,)), dma((KZ,)),
            dma((KZL,)), dma((KZL,)),
            dma((KZ,)), dma((KZ,)),
            dma((3, 4)),
        ],
        compiler_params=pltpu.CompilerParams(
            collective_id=0, has_side_effects=True, vmem_limit_bytes=48500000
        ),
        name="block_step",
    )(a_window, l_panel, l_inverse)


def solution(mesh):
    placed = (P("row", "col"), P("row", None), P())
    return jax.shard_map(
        body, mesh=mesh, in_specs=placed, out_specs=P("row", "col"), check_vma=False
    )
```

```python
import jax
import jax.numpy as jnp
from jax import lax
from jax.experimental import pallas as pl
from jax.experimental.pallas import tpu as pltpu
from jax.sharding import PartitionSpec as P

MESH = pl.DeviceIdType.MESH
F32 = jnp.float32
BF16 = jnp.bfloat16

W = 1024
HB = 512
RC = 8
KT = W // (4 * RC)
RP = 8
KP = W // (4 * RP)
RL = 16
KL = HB // (4 * RL)
ZR = 16
KZ = HB // ZR
RZ = 32
KZL = HB // 2 // RZ
SIG = 6
SP = 9
SZ = 6
SD = 2
ZL0 = 36
ZG0 = 62
DEEP = 6
HOLD = 48


def split(v):
    hi = v.astype(BF16)
    return hi, (v - hi.astype(F32)).astype(BF16)


def nn(a, b):
    return jnp.dot(a, b, preferred_element_type=F32)


def mul3(a, b):
    return nn(a[0], b[0]) + (nn(a[0], b[1]) + nn(a[1], b[0]))


def wrap(v):
    return lax.rem(v + 4, 4)


class Tree:
    def __init__(self, t, x, y, root):
        rx, ry = lax.rem(root, 4), lax.div(root, 4)
        sgn = 1 if t % 2 == 0 else -1
        dx, dy = wrap((x - rx) * sgn), wrap((y - ry) * sgn)
        main, sec = (dx, dy) if t < 2 else (dy, dx)
        self.depth = jnp.where(main == 0, jnp.where(sec == 0, 0, sec + 2), main + sec)
        self.root = jnp.logical_and(main == 0, sec == 0)
        step = jnp.where(sec == 0, sgn, -sgn)
        self.has = (
            jnp.logical_or(
                jnp.logical_and(sec == 0, main < 3), jnp.logical_and(sec > 0, main == 1)
            ),
            jnp.logical_and(main >= 1, sec < 3),
        )
        if t < 2:
            self.to = (y * 4 + wrap(x + step), wrap(y + sgn) * 4 + x)
        else:
            self.to = (wrap(y + step) * 4 + x, y * 4 + wrap(x + sgn))


def kernel(
    a_hbm, l_hbm, inv, u,
    big, lr, l10, gbuf, ph, plo, ah, al, lh, ll, ih, il, jh, jl, lth, ltl, mth, mtl,
    load_sem, tree_recv, tree_send, l10_send,
    zr1, zr2, lr1, lr2, gr1, gr2, zsend,
):
    row, col = lax.axis_index("row"), lax.axis_index("col")
    x, y = lax.rem(row, 4), lax.div(row, 4)
    z, core = lax.div(col, 2), lax.rem(col, 2)
    other = col + 1 - 2 * core
    top = row == 0

    def remote(src, dst, send, recv, to):
        return pltpu.make_async_remote_copy(
            src_ref=src, dst_ref=dst, send_sem=send, recv_sem=recv,
            device_id=to, device_id_type=MESH,
        )

    def rows_of(ref, at, n):
        return ref.at[pl.ds(pl.multiple_of(at, 8), n)]

    load_l = pltpu.make_async_copy(l_hbm, lr, load_sem.at[1])
    load_a = pltpu.make_async_copy(a_hbm, big.at[pl.ds(2 * W, W)], load_sem.at[2])
    load_u = pltpu.make_async_copy(a_hbm, u, load_sem.at[2])
    load_c = pltpu.make_async_copy(
        l_hbm.at[pl.ds(HB, HB), pl.ds(0, HB)], l10, load_sem.at[3]
    )
    load_t = pltpu.make_async_copy(a_hbm, big.at[pl.ds(0, W)], load_sem.at[4])
    load_r = pltpu.make_async_copy(l_hbm, big.at[pl.ds(0, W)], load_sem.at[4])
    panel = col == 0
    mine = row == col

    @pl.when(jnp.logical_and(mine, panel))
    def _():
        load_c.start()
        load_t.start()

    @pl.when(jnp.logical_and(mine, jnp.logical_not(panel)))
    def _():
        load_r.start()

    @pl.when(panel)
    def _():
        load_a.start()

    @pl.when(jnp.logical_not(panel))
    def _():
        load_u.start()

    load_l.start()

    barrier = pltpu.get_barrier_semaphore()
    peers = [
        (y * 4 + wrap(x + 1), col), (y * 4 + wrap(x - 1), col),
        (wrap(y + 1) * 4 + x, col), (wrap(y - 1) * 4 + x, col),
        (row, other),
        (row, 2 * wrap(z + 1) + core), (row, 2 * wrap(z - 1) + core),
        (row, 2 * wrap(z + jnp.where(core == 0, -1, 1)) + 1 - core),
    ]
    for peer in peers:
        pl.semaphore_signal(barrier, inc=1, device_id=peer, device_id_type=MESH)
    pl.semaphore_wait(barrier, len(peers))

    trees = [Tree(t, x, y, col) for t in range(4)]

    def split_inverse():
        for b in range(2):
            h, l = split(inv[b])
            ih[b] = h
            il[b] = l

    def split_coupling():
        h, l = split(l10[...])
        lth[...] = h
        ltl[...] = l

    def tree_step(t, k, at, buf, n, send):
        tree = trees[t]
        ref = rows_of(buf, at, n)

        @pl.when(jnp.logical_not(tree.root))
        def _():
            remote(ref, ref, send.at[t, 0], tree_recv.at[t, k], (row, col)).wait_recv()

        for s in range(2):
            @pl.when(tree.has[s])
            def _():
                remote(ref, ref, send.at[t, s], tree_recv.at[t, k], (tree.to[s], col)).start()

    def p_rows(at, n, eye):
        rows = pl.ds(pl.multiple_of(at, 8), n)
        l0, l1 = lr[rows, :HB], lr[rows, HB:]
        if eye:
            i = at + lax.broadcasted_iota(jnp.int32, (n, HB), 0)
            j = lax.broadcasted_iota(jnp.int32, (n, HB), 1)
            l0 = jnp.where(top, jnp.where(i == j, 1.0, 0.0), l0)
            l1 = jnp.where(top, jnp.where(i == j + HB, 1.0, 0.0), l1)
        p1 = split(mul3(split(l1), (ih[1], il[1])))
        ph[rows, HB:] = p1[0]
        plo[rows, HB:] = p1[1]
        p0 = split(
            mul3(split(l0 - mul3(p1, (lth[...], ltl[...]))), (ih[0], il[0]))
        )
        ph[rows, :HB] = p0[0]
        plo[rows, :HB] = p0[1]

    def right_solve(r, put):
        x0 = mul3(split(r[:, :HB]), (jh[0], jl[0]))
        put(0, x0)
        mid = r[:, HB:] - mul3(split(x0), (mth[...], mtl[...]))
        put(HB, mul3(split(mid), (jh[1], jl[1])))

    @pl.when(col == 0)
    def _():
        @pl.when(top)
        def _():
            load_c.wait()
            load_t.wait()

        def send_a(k, _):
            @pl.when(row >= 2)
            def _():
                for half, to in ((0, 2), (1, 7)):
                    src = rows_of(big, 2 * W + half * HB + k * ZR, ZR)
                    at = jnp.where(row == to, W, 2 * W)
                    dst = rows_of(big, at + half * HB + k * ZR, ZR)
                    remote(src, dst, zsend.at[0, half], zr1.at[k], (row, to)).start()

            @pl.when(row == 1)
            def _():
                for half, recv in ((0, zr2), (1, zr1)):
                    src = rows_of(big, 2 * W + half * HB + k * ZR, ZR)
                    dst = rows_of(big, W + half * HB + k * ZR, ZR)
                    remote(src, dst, zsend.at[0, 2 + half], recv.at[k], (row, 1)).start()
            return 0


        def slot(s):
            for t in range(4):
                k = s - SP * trees[t].depth

                @pl.when(jnp.logical_and(k >= 0, k < KL))
                def _():
                    tree_step(t, k, (k * 4 + t) * RL, l10, RL, l10_send)

                k2 = k - KL

                @pl.when(jnp.logical_and(k2 >= 0, k2 < KP))
                def _():
                    tree_step(t, k2 + KL, (k2 * 4 + t) * RP, big, RP, tree_send)

        first = KL + SP * DEEP

        def comm_only(s, _):
            slot(s)
            return 0

        lax.fori_loop(0, 4, comm_only, 0)
        load_a.wait()

        def with_send(i, _):
            slot(4 + i)

            @pl.when(jnp.logical_and(row >= 2, row < 8))
            def _():
                lax.fori_loop(2 * i, 2 * i + 2, send_a, 0)
            return 0

        lax.fori_loop(0, KZ // 2, with_send, 0)
        split_inverse()
        lax.fori_loop(20, 24, comm_only, 0)
        for b in range(2):
            h, l = split(inv[b].T)
            jh[b] = h
            jl[b] = l
        load_l.wait()
        lax.fori_loop(24, HOLD, comm_only, 0)

        @pl.when(row == 1)
        def _():
            lax.fori_loop(0, KZ, send_a, 0)

        lax.fori_loop(HOLD, first, comm_only, 0)

        def send_l(k, _):
            for half, to in ((0, 2), (1, 7)):
                ref = rows_of(l10, half * (HB // 2) + k * RZ, RZ)
                remote(ref, ref, zsend.at[1, half], lr1.at[k], (row, to)).start()
            for half, recv in ((0, lr2), (1, lr1)):
                ref = rows_of(l10, half * (HB // 2) + k * RZ, RZ)
                remote(ref, ref, zsend.at[1, 2 + half], recv.at[k], (row, 1)).start()
            return 0

        lax.fori_loop(0, KZL, send_l, 0)
        split_coupling()
        h, l = split(l10[...].T)
        mth[...] = h
        mtl[...] = l

        def with_p(i, _):
            for j in range(4):
                slot(first + 4 * i + j)
            p_rows(i * 128, 128, True)
            return 0

        lax.fori_loop(0, 8, with_p, 0)
        lax.fori_loop(first + 32, KL + KP + SP * DEEP, comm_only, 0)

        def split_t(i, _):
            rows = pl.ds(pl.multiple_of(i * 128, 128), 128)
            h, l = split(big[pl.ds(pl.multiple_of(i * 128, 128), 128)] + big[0:W, rows].T)
            lh[rows] = h
            ll[rows] = l
            return 0

        lax.fori_loop(0, 8, split_t, 0)

        def place(g):
            half, q = lax.rem(g, 2), lax.div(g, 2)
            return half, q, half * HB + q * 128

        def send_block(g):
            half, q, at = place(g)

            def send_g(j, _):
                ref = rows_of(gbuf, at + j * ZR, ZR)
                k = q * (128 // ZR) + j

                @pl.when(half == 0)
                def _():
                    remote(ref, ref, zsend.at[2, 0], gr1.at[k], (row, 2)).start()
                    remote(ref, ref, zsend.at[2, 2], gr2.at[k], (row, 1)).start()

                @pl.when(half == 1)
                def _():
                    remote(ref, ref, zsend.at[2, 1], gr1.at[k], (row, 7)).start()
                    remote(ref, ref, zsend.at[2, 3], gr1.at[k], (row, 1)).start()
                return 0

            lax.fori_loop(0, 128 // ZR, send_g, 0)

        def g_block(g, _):
            _, _, at = place(g)
            rows = pl.ds(pl.multiple_of(at, 128), 128)
            p = (ph[rows], plo[rows])

            def part(n):
                cols = slice(n * HB, n * HB + HB)
                pt = mul3(p, (lh[:, cols], ll[:, cols]))
                a = big[pl.ds(pl.multiple_of(2 * W + at, 128), 128), cols]
                gbuf[rows, cols] = a - 0.5 * pt

            part(0)

            @pl.when(g > 0)
            def _():
                send_block(g - 1)

            part(1)

            def put_g(c0, v):
                gbuf[rows, c0:c0 + HB] = v

            right_solve(gbuf[rows], put_g)
            return 0

        lax.fori_loop(0, 8, g_block, 0)

        def split_a(i, _):
            rows = pl.ds(pl.multiple_of(i * 128, 128), 128)
            h, l = split(big[rows])
            ah[rows] = h
            al[rows] = l
            return 0

        lax.fori_loop(0, 8, split_a, 0)
        send_block(7)

        def o_block(g, _):
            rows = pl.ds(pl.multiple_of(g * 128, 128), 128)
            p = (ph[rows], plo[rows])
            for n in range(2):
                cols = slice(n * HB, n * HB + HB)
                e = mul3(p, (ah[:, cols], al[:, cols]))
                a = big[pl.ds(pl.multiple_of(2 * W + g * 128, 128), 128), cols]
                u[rows, cols] = jnp.where(top, e, a - e)

            def put_o(c0, v):
                u[rows, c0:c0 + HB] = v

            right_solve(u[rows], put_o)
            return 0

        lax.fori_loop(0, 4, o_block, 0)
        lax.fori_loop(4, 8, o_block, 0)
        for t in range(4):
            for s in range(2):
                @pl.when(trees[t].has[s])
                def _():
                    ref = l10.at[pl.ds(0, KL * RL)]
                    remote(ref, ref, l10_send.at[t, s], lr1.at[0], (row, 1)).wait_send()
                    ref = big.at[pl.ds(0, KP * RP)]
                    remote(ref, ref, tree_send.at[t, s], lr1.at[0], (row, 1)).wait_send()
        for s in range(4):
            ref = big.at[pl.ds(0, HB)]
            @pl.when(jnp.logical_and(row >= 2, row < 8) if s < 2 else row == 1)
            def _():
                remote(ref, ref, zsend.at[0, s], lr1.at[0], (row, 1)).wait_send()

            remote(ref, ref, zsend.at[2, s], lr1.at[0], (row, 1)).wait_send()
            ref = l10.at[pl.ds(0, HB // 2)]
            remote(ref, ref, zsend.at[1, s], lr1.at[0], (row, 1)).wait_send()

    def trailing(one):
        rc, sig = (16, 5) if one else (RC, SIG)
        kt = W // (4 * rc)
        zl0, zg0 = (4, 30) if one else (ZL0, ZG0)
        have_l = zl0 + KZL + (SD if one else 3 * SZ + SD)
        per = kt // 4
        begin = (per if one else kt + per) + sig * DEEP
        a_at, g_at = (1, 2) if one else (1, 3), (5, 7)

        @pl.when(mine)
        def _():
            load_r.wait()

        far = z > 0
        zrow = jnp.logical_and(far, jnp.logical_and(row >= 2, row < 8))
        first_slots = jnp.where(far, SZ * jnp.where(core == 0, z, 4 - z), SD)
        second_slots = jnp.where(far, SZ * jnp.where(core == 0, 4 - z, z) + SD, SD)
        on = jnp.where(core == 0, jnp.logical_and(far, z < 3), z > 1)
        nxt = jnp.where(core == 0, col + 2, col - 2)
        half = jnp.where(core == 0, 0, 1)

        def z_step(s, begin, count, ref_of, first, second, kind, only_root):
            k = s - begin - first_slots

            @pl.when(jnp.logical_and(k >= 0, k < count))
            def _():
                def go():
                    src = ref_of(col, half, k)
                    remote(src, src, zsend.at[kind, 0], first.at[k], (row, col)).wait_recv()

                    @pl.when(on)
                    def _():
                        remote(
                            src, ref_of(nxt, half, k), zsend.at[kind, 0], first.at[k], (row, nxt)
                        ).start()

                    @pl.when(jnp.logical_and(far, row == other) if only_root else far)
                    def _():
                        remote(
                            src, ref_of(other, half, k), zsend.at[kind, 1], second.at[k],
                            (row, other),
                        ).start()

                if only_root:
                    pl.when(zrow)(go)
                else:
                    go()

            k2 = s - begin - second_slots

            @pl.when(jnp.logical_and(k2 >= 0, k2 < count))
            def _():
                def go():
                    src = ref_of(col, 1 - half, k2)
                    remote(src, src, zsend.at[kind, 1], second.at[k2], (row, col)).wait_recv()

                if only_root:
                    pl.when(jnp.logical_and(zrow, mine))(go)
                else:
                    go()

        def a_ref(c, h, k):
            base = jnp.where(row == c, W, 2 * W)
            return rows_of(big, base + h * HB + k * ZR, ZR)

        def l_ref(c, h, k):
            return rows_of(l10, h * (HB // 2) + k * RZ, RZ)

        def g_ref(c, h, k):
            return rows_of(gbuf, h * HB + k * ZR, ZR)

        if one:
            @pl.when(mine)
            def _():
                def arrive(k, _):
                    ref = rows_of(big, W + k * ZR, ZR)
                    remote(ref, ref, zsend.at[0, 0], zr1.at[k], (row, col)).wait_recv()
                    remote(ref, ref, zsend.at[0, 0], zr2.at[k], (row, col)).wait_recv()
                    return 0

                lax.fori_loop(0, KZ, arrive, 0)

        def slot(s):
            if not one:
                z_step(s, 0, KZ, a_ref, zr1, zr2, 0, True)
            z_step(s, zl0, KZL, l_ref, lr1, lr2, 1, False)
            z_step(s, zg0, KZ, g_ref, gr1, gr2, 2, False)
            for t in range(4):
                k = s - sig * trees[t].depth

                @pl.when(jnp.logical_and(k >= 0, k < 2 * kt))
                def _():
                    m, i = lax.div(k, kt), lax.rem(k, kt)
                    at = (1 - m if one else m) * W + (t // 2) * HB + i * 2 * rc + (t % 2) * rc
                    tree_step(t, k, at, big, rc, tree_send)

        def comm_only(s, _):
            slot(s)
            return 0

        early = min(20, have_l)
        lax.fori_loop(0, early, comm_only, 0)
        split_inverse()
        lax.fori_loop(early, have_l, comm_only, 0)
        split_coupling()
        load_l.wait()

        def with_p(i, _):
            slot(have_l + 2 * i)
            slot(have_l + 2 * i + 1)
            p_rows(i * 256, 256, False)
            return 0

        lax.fori_loop(0, 4, with_p, 0)
        assert have_l + (8 if one else 12) <= begin
        lax.fori_loop(have_l + 8, begin - (0 if one else 4), comm_only, 0)
        load_u.wait()

        def split_l(i, _):
            slot(begin - 4 + i)
            for j in range(2):
                at = i * 256 + j * 128
                cols = pl.ds(pl.multiple_of(at, 128), 128)
                h, l = split(big[pl.ds(pl.multiple_of(at, 128), 128)].T)
                lh[:, cols] = h
                ll[:, cols] = l
            return 0

        if not one:
            lax.fori_loop(0, 4, split_l, 0)

        def split_g(g):
            for j in range(2):
                rows = pl.ds(pl.multiple_of(j * HB + g * 128, 128), 128)
                h, l = split(gbuf[rows])
                ph[rows] = h
                plo[rows] = l

        def with_update(v, _):
            slot(begin + v)
            b, w = lax.div(v, per), lax.rem(v, per)

            @pl.when(jnp.logical_and(w == 0, b < 4))
            def _():
                for j in range(2):
                    at = W + j * HB + b * 128
                    h, l = split(big[pl.ds(pl.multiple_of(at, 128), 128)].T)
                    ah[:, j * 128:j * 128 + 128] = h
                    al[:, j * 128:j * 128 + 128] = l

            @pl.when(jnp.logical_and(jnp.logical_or(w == a_at[0], w == a_at[1]), b < 4))
            def _():
                rows = pl.ds(pl.multiple_of(jnp.where(w == a_at[1], HB, 0), HB), HB)
                upd = mul3((ph[rows], plo[rows]), (ah[:, 0:256], al[:, 0:256]))
                for j in range(2):
                    cols = pl.ds(pl.multiple_of(j * HB + b * 128, 128), 128)
                    part = jnp.where(top, 0.0, upd[:, j * 128:j * 128 + 128])
                    u[rows, cols] = u[rows, cols] - part

            if one:
                @pl.when(jnp.logical_and(w == 0, b >= 4))
                def _():
                    for j in range(2):
                        at = j * HB + (b - 4) * 128
                        cols = pl.ds(pl.multiple_of((b - 4) * 256 + j * 128, 128), 128)
                        h, l = split(big[pl.ds(pl.multiple_of(at, 128), 128)].T)
                        lh[:, cols] = h
                        ll[:, cols] = l

                @pl.when(jnp.logical_and(w == 1, jnp.logical_and(b >= 4, b < 7)))
                def _():
                    split_g(b - 4)
            else:
                gb = b - 1

                @pl.when(jnp.logical_and(jnp.logical_or(w == g_at[0], w == g_at[1]), gb >= 0))
                def _():
                    at = jnp.where(w == g_at[1], HB, 0) + gb * 128
                    rows = pl.ds(pl.multiple_of(at, 128), 128)
                    g = split(gbuf[rows])
                    for j in range(2):
                        cols = slice(j * HB, j * HB + HB)
                        upd = mul3(g, (lh[:, cols], ll[:, cols]))
                        u[rows, cols] = u[rows, cols] - jnp.where(top, 0.0, upd)
            return 0

        lax.fori_loop(0, per * (8 if one else 5), with_update, 0)

        if one:
            split_g(3)

            def g_update(i, _):
                n, h = lax.div(i, 2), lax.rem(i, 2)
                rows = pl.ds(pl.multiple_of(h * HB, HB), HB)
                cols = pl.ds(pl.multiple_of(n * 256, 256), 256)
                upd = mul3((ph[rows], plo[rows]), (lh[:, cols], ll[:, cols]))
                for j in range(2):
                    at = pl.ds(pl.multiple_of(j * HB + n * 128, 128), 128)
                    part = jnp.where(top, 0.0, upd[:, j * 128:j * 128 + 128])
                    u[rows, at] = u[rows, at] - part
                return 0

            lax.fori_loop(0, 8, g_update, 0)
        for t in range(4):
            for s in range(2):
                @pl.when(trees[t].has[s])
                def _():
                    ref = big.at[pl.ds(0, HB)]
                    remote(ref, ref, tree_send.at[t, s], lr1.at[0], (row, col)).wait_send()
        for kind in range(3):
            ref = l10.at[pl.ds(0, HB // 2)] if kind == 1 else big.at[pl.ds(0, HB)]

            @pl.when(jnp.logical_and(zrow, on) if kind == 0 else on)
            def _():
                remote(ref, ref, zsend.at[kind, 0], lr1.at[0], (row, col)).wait_send()

            @pl.when(jnp.logical_and(zrow, row == other) if kind == 0 else far)
            def _():
                remote(ref, ref, zsend.at[kind, 1], lr1.at[0], (row, col)).wait_send()


    @pl.when(col == 1)
    def _():
        trailing(True)

    @pl.when(col > 1)
    def _():
        trailing(False)


def body(a_window, l_panel, l_inverse):
    vmem = pltpu.VMEM
    dma = pltpu.SemaphoreType.DMA
    return pl.pallas_call(
        kernel,
        out_shape=jax.ShapeDtypeStruct((W, W), F32),
        in_specs=[pl.BlockSpec(memory_space=pl.ANY)] * 2 + [pl.BlockSpec(memory_space=pltpu.VMEM)],
        out_specs=pl.BlockSpec(memory_space=pltpu.VMEM),
        scratch_shapes=[
            vmem((3 * W, W), F32),
            vmem((W, W), F32),
            vmem((HB, HB), F32),
            vmem((W, W), F32),
            vmem((W, W), BF16), vmem((W, W), BF16),
            vmem((W, W), BF16), vmem((W, W), BF16),
            vmem((W, W), BF16), vmem((W, W), BF16),
            vmem((2, HB, HB), BF16), vmem((2, HB, HB), BF16),
            vmem((2, HB, HB), BF16), vmem((2, HB, HB), BF16),
            vmem((HB, HB), BF16), vmem((HB, HB), BF16),
            vmem((HB, HB), BF16), vmem((HB, HB), BF16),
            dma((5,)),
            dma((4, 2 * KT)),
            dma((4, 2)),
            dma((4, 2)),
            dma((KZ,)), dma((KZ,)),
            dma((KZL,)), dma((KZL,)),
            dma((KZ,)), dma((KZ,)),
            dma((3, 4)),
        ],
        compiler_params=pltpu.CompilerParams(
            collective_id=0, has_side_effects=True, vmem_limit_bytes=48500000
        ),
        name="block_step",
    )(a_window, l_panel, l_inverse)


def solution(mesh):
    placed = (P("row", "col"), P("row", None), P())
    return jax.shard_map(
        body, mesh=mesh, in_specs=placed, out_specs=P("row", "col"), check_vma=False
    )
```

```python
import jax
import jax.numpy as jnp
from jax import lax
from jax.experimental import pallas as pl
from jax.experimental.pallas import tpu as pltpu
from jax.sharding import PartitionSpec as P

MESH = pl.DeviceIdType.MESH
F32 = jnp.float32
BF16 = jnp.bfloat16

W = 1024
HB = 512
RC = 8
KT = W // (4 * RC)
RP = 8
KP = W // (4 * RP)
RL = 16
KL = HB // (4 * RL)
ZR = 16
KZ = HB // ZR
RZ = 32
KZL = HB // 2 // RZ
SIG = 6
SP = 9
SZ = 6
SD = 2
ZL0 = 36
ZG0 = 62
DEEP = 6
HOLD = 48


def split(v):
    hi = v.astype(BF16)
    return hi, (v - hi.astype(F32)).astype(BF16)


def nn(a, b):
    return jnp.dot(a, b, preferred_element_type=F32)


def mul3(a, b):
    return nn(a[0], b[0]) + (nn(a[0], b[1]) + nn(a[1], b[0]))


def wrap(v):
    return lax.rem(v + 4, 4)


class Tree:
    def __init__(self, t, x, y, root):
        rx, ry = lax.rem(root, 4), lax.div(root, 4)
        sgn = 1 if t % 2 == 0 else -1
        dx, dy = wrap((x - rx) * sgn), wrap((y - ry) * sgn)
        main, sec = (dx, dy) if t < 2 else (dy, dx)
        self.depth = jnp.where(main == 0, jnp.where(sec == 0, 0, sec + 2), main + sec)
        self.root = jnp.logical_and(main == 0, sec == 0)
        step = jnp.where(sec == 0, sgn, -sgn)
        self.has = (
            jnp.logical_or(
                jnp.logical_and(sec == 0, main < 3), jnp.logical_and(sec > 0, main == 1)
            ),
            jnp.logical_and(main >= 1, sec < 3),
        )
        if t < 2:
            self.to = (y * 4 + wrap(x + step), wrap(y + sgn) * 4 + x)
        else:
            self.to = (wrap(y + step) * 4 + x, y * 4 + wrap(x + sgn))


def kernel(
    a_hbm, l_hbm, inv, u,
    big, lr, l10, gbuf, ph, plo, ah, al, lh, ll, ih, il, jh, jl, lth, ltl, mth, mtl,
    load_sem, tree_recv, tree_send, l10_send,
    zr1, zr2, lr1, lr2, gr1, gr2, zsend,
):
    row, col = lax.axis_index("row"), lax.axis_index("col")
    x, y = lax.rem(row, 4), lax.div(row, 4)
    z, core = lax.div(col, 2), lax.rem(col, 2)
    other = col + 1 - 2 * core
    top = row == 0

    def remote(src, dst, send, recv, to):
        return pltpu.make_async_remote_copy(
            src_ref=src, dst_ref=dst, send_sem=send, recv_sem=recv,
            device_id=to, device_id_type=MESH,
        )

    def rows_of(ref, at, n):
        return ref.at[pl.ds(pl.multiple_of(at, 8), n)]

    load_l = pltpu.make_async_copy(l_hbm, lr, load_sem.at[1])
    load_a = pltpu.make_async_copy(a_hbm, big.at[pl.ds(2 * W, W)], load_sem.at[2])
    load_u = pltpu.make_async_copy(a_hbm, u, load_sem.at[2])
    load_c = pltpu.make_async_copy(
        l_hbm.at[pl.ds(HB, HB), pl.ds(0, HB)], l10, load_sem.at[3]
    )
    load_t = pltpu.make_async_copy(a_hbm, big.at[pl.ds(0, W)], load_sem.at[4])
    load_r = pltpu.make_async_copy(l_hbm, big.at[pl.ds(0, W)], load_sem.at[4])
    panel = col == 0
    mine = row == col

    @pl.when(jnp.logical_and(mine, panel))
    def _():
        load_c.start()
        load_t.start()

    @pl.when(jnp.logical_and(mine, jnp.logical_not(panel)))
    def _():
        load_r.start()

    @pl.when(panel)
    def _():
        load_a.start()

    @pl.when(jnp.logical_not(panel))
    def _():
        load_u.start()

    load_l.start()

    barrier = pltpu.get_barrier_semaphore()
    peers = [
        (y * 4 + wrap(x + 1), col), (y * 4 + wrap(x - 1), col),
        (wrap(y + 1) * 4 + x, col), (wrap(y - 1) * 4 + x, col),
        (row, other),
        (row, 2 * wrap(z + 1) + core), (row, 2 * wrap(z - 1) + core),
        (row, 2 * wrap(z + jnp.where(core == 0, -1, 1)) + 1 - core),
    ]
    for peer in peers:
        pl.semaphore_signal(barrier, inc=1, device_id=peer, device_id_type=MESH)
    pl.semaphore_wait(barrier, len(peers))

    trees = [Tree(t, x, y, col) for t in range(4)]

    def split_inverse():
        for b in range(2):
            h, l = split(inv[b])
            ih[b] = h
            il[b] = l

    def split_coupling():
        h, l = split(l10[...])
        lth[...] = h
        ltl[...] = l

    def tree_step(t, k, at, buf, n, send):
        tree = trees[t]
        ref = rows_of(buf, at, n)

        @pl.when(jnp.logical_not(tree.root))
        def _():
            remote(ref, ref, send.at[t, 0], tree_recv.at[t, k], (row, col)).wait_recv()

        for s in range(2):
            @pl.when(tree.has[s])
            def _():
                remote(ref, ref, send.at[t, s], tree_recv.at[t, k], (tree.to[s], col)).start()

    def p_rows(at, n, eye):
        rows = pl.ds(pl.multiple_of(at, 8), n)
        l0, l1 = lr[rows, :HB], lr[rows, HB:]
        if eye:
            i = at + lax.broadcasted_iota(jnp.int32, (n, HB), 0)
            j = lax.broadcasted_iota(jnp.int32, (n, HB), 1)
            l0 = jnp.where(top, jnp.where(i == j, 1.0, 0.0), l0)
            l1 = jnp.where(top, jnp.where(i == j + HB, 1.0, 0.0), l1)
        p1 = split(mul3(split(l1), (ih[1], il[1])))
        ph[rows, HB:] = p1[0]
        plo[rows, HB:] = p1[1]
        p0 = split(
            mul3(split(l0 - mul3(p1, (lth[...], ltl[...]))), (ih[0], il[0]))
        )
        ph[rows, :HB] = p0[0]
        plo[rows, :HB] = p0[1]

    def right_solve(r, put):
        x0 = mul3(split(r[:, :HB]), (jh[0], jl[0]))
        put(0, x0)
        mid = r[:, HB:] - mul3(split(x0), (mth[...], mtl[...]))
        put(HB, mul3(split(mid), (jh[1], jl[1])))

    @pl.when(col == 0)
    def _():
        @pl.when(top)
        def _():
            load_c.wait()
            load_t.wait()

        def send_a(k, _):
            @pl.when(row >= 2)
            def _():
                for half, to in ((0, 2), (1, 7)):
                    src = rows_of(big, 2 * W + half * HB + k * ZR, ZR)
                    at = jnp.where(row == to, W, 2 * W)
                    dst = rows_of(big, at + half * HB + k * ZR, ZR)
                    remote(src, dst, zsend.at[0, half], zr1.at[k], (row, to)).start()

            @pl.when(row == 1)
            def _():
                for half, recv in ((0, zr2), (1, zr1)):
                    src = rows_of(big, 2 * W + half * HB + k * ZR, ZR)
                    dst = rows_of(big, W + half * HB + k * ZR, ZR)
                    remote(src, dst, zsend.at[0, 2 + half], recv.at[k], (row, 1)).start()
            return 0


        def slot(s):
            for t in range(4):
                k = s - SP * trees[t].depth

                @pl.when(jnp.logical_and(k >= 0, k < KL))
                def _():
                    tree_step(t, k, (k * 4 + t) * RL, l10, RL, l10_send)

                k2 = k - KL

                @pl.when(jnp.logical_and(k2 >= 0, k2 < KP))
                def _():
                    tree_step(t, k2 + KL, (k2 * 4 + t) * RP, big, RP, tree_send)

        first = KL + SP * DEEP

        def comm_only(s, _):
            slot(s)
            return 0

        lax.fori_loop(0, 4, comm_only, 0)
        load_a.wait()

        def with_send(i, _):
            slot(4 + i)

            @pl.when(jnp.logical_and(row >= 2, row < 8))
            def _():
                lax.fori_loop(2 * i, 2 * i + 2, send_a, 0)
            return 0

        lax.fori_loop(0, KZ // 2, with_send, 0)
        split_inverse()
        lax.fori_loop(20, 24, comm_only, 0)
        for b in range(2):
            h, l = split(inv[b].T)
            jh[b] = h
            jl[b] = l
        load_l.wait()
        lax.fori_loop(24, HOLD, comm_only, 0)

        @pl.when(row == 1)
        def _():
            lax.fori_loop(0, KZ, send_a, 0)

        lax.fori_loop(HOLD, first, comm_only, 0)

        def send_l(k, _):
            for half, to in ((0, 2), (1, 7)):
                ref = rows_of(l10, half * (HB // 2) + k * RZ, RZ)
                remote(ref, ref, zsend.at[1, half], lr1.at[k], (row, to)).start()
            for half, recv in ((0, lr2), (1, lr1)):
                ref = rows_of(l10, half * (HB // 2) + k * RZ, RZ)
                remote(ref, ref, zsend.at[1, 2 + half], recv.at[k], (row, 1)).start()
            return 0

        lax.fori_loop(0, KZL, send_l, 0)
        split_coupling()
        h, l = split(l10[...].T)
        mth[...] = h
        mtl[...] = l

        def with_p(i, _):
            for j in range(4):
                slot(first + 4 * i + j)
            p_rows(i * 128, 128, True)
            return 0

        lax.fori_loop(0, 8, with_p, 0)
        lax.fori_loop(first + 32, KL + KP + SP * DEEP, comm_only, 0)

        def split_t(i, _):
            rows = pl.ds(pl.multiple_of(i * 128, 128), 128)
            h, l = split(big[pl.ds(pl.multiple_of(i * 128, 128), 128)] + big[0:W, rows].T)
            lh[rows] = h
            ll[rows] = l
            return 0

        lax.fori_loop(0, 8, split_t, 0)

        def place(g):
            half, q = lax.rem(g, 2), lax.div(g, 2)
            return half, q, half * HB + q * 128

        def send_block(g):
            half, q, at = place(g)

            def send_g(j, _):
                ref = rows_of(gbuf, at + j * ZR, ZR)
                k = q * (128 // ZR) + j

                @pl.when(half == 0)
                def _():
                    remote(ref, ref, zsend.at[2, 0], gr1.at[k], (row, 2)).start()
                    remote(ref, ref, zsend.at[2, 2], gr2.at[k], (row, 1)).start()

                @pl.when(half == 1)
                def _():
                    remote(ref, ref, zsend.at[2, 1], gr1.at[k], (row, 7)).start()
                    remote(ref, ref, zsend.at[2, 3], gr1.at[k], (row, 1)).start()
                return 0

            lax.fori_loop(0, 128 // ZR, send_g, 0)

        def g_block(g, _):
            _, _, at = place(g)
            rows = pl.ds(pl.multiple_of(at, 128), 128)
            p = (ph[rows], plo[rows])

            def part(n):
                cols = slice(n * HB, n * HB + HB)
                pt = mul3(p, (lh[:, cols], ll[:, cols]))
                a = big[pl.ds(pl.multiple_of(2 * W + at, 128), 128), cols]
                gbuf[rows, cols] = a - 0.5 * pt

            part(0)

            @pl.when(g > 0)
            def _():
                send_block(g - 1)

            part(1)

            def put_g(c0, v):
                gbuf[rows, c0:c0 + HB] = v

            right_solve(gbuf[rows], put_g)
            return 0

        lax.fori_loop(0, 8, g_block, 0)

        def split_a(i, _):
            rows = pl.ds(pl.multiple_of(i * 128, 128), 128)
            h, l = split(big[rows])
            ah[rows] = h
            al[rows] = l
            return 0

        lax.fori_loop(0, 8, split_a, 0)
        send_block(7)

        def o_block(g, _):
            rows = pl.ds(pl.multiple_of(g * 128, 128), 128)
            p = (ph[rows], plo[rows])
            for n in range(2):
                cols = slice(n * HB, n * HB + HB)
                e = mul3(p, (ah[:, cols], al[:, cols]))
                a = big[pl.ds(pl.multiple_of(2 * W + g * 128, 128), 128), cols]
                u[rows, cols] = jnp.where(top, e, a - e)

            def put_o(c0, v):
                u[rows, c0:c0 + HB] = v

            right_solve(u[rows], put_o)
            return 0

        lax.fori_loop(0, 4, o_block, 0)
        lax.fori_loop(4, 8, o_block, 0)
        for t in range(4):
            for s in range(2):
                @pl.when(trees[t].has[s])
                def _():
                    ref = l10.at[pl.ds(0, KL * RL)]
                    remote(ref, ref, l10_send.at[t, s], lr1.at[0], (row, 1)).wait_send()
                    ref = big.at[pl.ds(0, KP * RP)]
                    remote(ref, ref, tree_send.at[t, s], lr1.at[0], (row, 1)).wait_send()
        for s in range(4):
            ref = big.at[pl.ds(0, HB)]
            @pl.when(jnp.logical_and(row >= 2, row < 8) if s < 2 else row == 1)
            def _():
                remote(ref, ref, zsend.at[0, s], lr1.at[0], (row, 1)).wait_send()

            remote(ref, ref, zsend.at[2, s], lr1.at[0], (row, 1)).wait_send()
            ref = l10.at[pl.ds(0, HB // 2)]
            remote(ref, ref, zsend.at[1, s], lr1.at[0], (row, 1)).wait_send()

    def trailing(one):
        rc, sig = (16, 5) if one else (RC, SIG)
        kt = W // (4 * rc)
        zl0, zg0 = (4, 30) if one else (ZL0, ZG0)
        have_l = zl0 + KZL + (SD if one else 3 * SZ + SD)
        per = kt // 4
        begin = (per if one else kt + per) + sig * DEEP
        a_at, g_at = (1, 2) if one else (1, 3), (5, 7)

        @pl.when(mine)
        def _():
            load_r.wait()

        far = z > 0
        zrow = jnp.logical_and(far, jnp.logical_and(row >= 2, row < 8))
        first_slots = jnp.where(far, SZ * jnp.where(core == 0, z, 4 - z), SD)
        second_slots = jnp.where(far, SZ * jnp.where(core == 0, 4 - z, z) + SD, SD)
        on = jnp.where(core == 0, jnp.logical_and(far, z < 3), z > 1)
        nxt = jnp.where(core == 0, col + 2, col - 2)
        half = jnp.where(core == 0, 0, 1)

        def z_step(s, begin, count, ref_of, first, second, kind, only_root):
            k = s - begin - first_slots

            @pl.when(jnp.logical_and(k >= 0, k < count))
            def _():
                def go():
                    src = ref_of(col, half, k)
                    remote(src, src, zsend.at[kind, 0], first.at[k], (row, col)).wait_recv()

                    @pl.when(on)
                    def _():
                        remote(
                            src, ref_of(nxt, half, k), zsend.at[kind, 0], first.at[k], (row, nxt)
                        ).start()

                    @pl.when(jnp.logical_and(far, row == other) if only_root else far)
                    def _():
                        remote(
                            src, ref_of(other, half, k), zsend.at[kind, 1], second.at[k],
                            (row, other),
                        ).start()

                if only_root:
                    pl.when(zrow)(go)
                else:
                    go()

            k2 = s - begin - second_slots

            @pl.when(jnp.logical_and(k2 >= 0, k2 < count))
            def _():
                def go():
                    src = ref_of(col, 1 - half, k2)
                    remote(src, src, zsend.at[kind, 1], second.at[k2], (row, col)).wait_recv()

                if only_root:
                    pl.when(jnp.logical_and(zrow, mine))(go)
                else:
                    go()

        def a_ref(c, h, k):
            base = jnp.where(row == c, W, 2 * W)
            return rows_of(big, base + h * HB + k * ZR, ZR)

        def l_ref(c, h, k):
            return rows_of(l10, h * (HB // 2) + k * RZ, RZ)

        def g_ref(c, h, k):
            return rows_of(gbuf, h * HB + k * ZR, ZR)

        if one:
            @pl.when(mine)
            def _():
                def arrive(k, _):
                    ref = rows_of(big, W + k * ZR, ZR)
                    remote(ref, ref, zsend.at[0, 0], zr1.at[k], (row, col)).wait_recv()
                    remote(ref, ref, zsend.at[0, 0], zr2.at[k], (row, col)).wait_recv()
                    return 0

                lax.fori_loop(0, KZ, arrive, 0)

        def slot(s):
            if not one:
                z_step(s, 0, KZ, a_ref, zr1, zr2, 0, True)
            z_step(s, zl0, KZL, l_ref, lr1, lr2, 1, False)
            z_step(s, zg0, KZ, g_ref, gr1, gr2, 2, False)
            for t in range(4):
                k = s - sig * trees[t].depth

                @pl.when(jnp.logical_and(k >= 0, k < 2 * kt))
                def _():
                    m, i = lax.div(k, kt), lax.rem(k, kt)
                    at = (1 - m if one else m) * W + (t // 2) * HB + i * 2 * rc + (t % 2) * rc
                    tree_step(t, k, at, big, rc, tree_send)

        def comm_only(s, _):
            slot(s)
            return 0

        early = min(20, have_l)
        lax.fori_loop(0, early, comm_only, 0)
        split_inverse()
        lax.fori_loop(early, have_l, comm_only, 0)
        split_coupling()
        load_l.wait()

        def with_p(i, _):
            slot(have_l + 2 * i)
            slot(have_l + 2 * i + 1)
            p_rows(i * 256, 256, False)
            return 0

        lax.fori_loop(0, 4, with_p, 0)
        assert have_l + (8 if one else 12) <= begin
        lax.fori_loop(have_l + 8, begin - (0 if one else 4), comm_only, 0)
        load_u.wait()

        def split_l(i, _):
            slot(begin - 4 + i)
            for j in range(2):
                at = i * 256 + j * 128
                cols = pl.ds(pl.multiple_of(at, 128), 128)
                h, l = split(big[pl.ds(pl.multiple_of(at, 128), 128)].T)
                lh[:, cols] = h
                ll[:, cols] = l
            return 0

        if not one:
            lax.fori_loop(0, 4, split_l, 0)

        def split_g(g):
            for j in range(2):
                rows = pl.ds(pl.multiple_of(j * HB + g * 128, 128), 128)
                h, l = split(gbuf[rows])
                ph[rows] = h
                plo[rows] = l

        def with_update(v, _):
            slot(begin + v)
            b, w = lax.div(v, per), lax.rem(v, per)

            @pl.when(jnp.logical_and(w == 0, b < 4))
            def _():
                for j in range(2):
                    at = W + j * HB + b * 128
                    h, l = split(big[pl.ds(pl.multiple_of(at, 128), 128)].T)
                    ah[:, j * 128:j * 128 + 128] = h
                    al[:, j * 128:j * 128 + 128] = l

            @pl.when(jnp.logical_and(w == a_at[0], b < 4))
            def _():
                rows = pl.ds(0, W)
                upd = mul3((ph[rows], plo[rows]), (ah[:, 0:256], al[:, 0:256]))
                for j in range(2):
                    cols = pl.ds(pl.multiple_of(j * HB + b * 128, 128), 128)
                    part = jnp.where(top, 0.0, upd[:, j * 128:j * 128 + 128])
                    u[rows, cols] = u[rows, cols] - part

            if one:
                @pl.when(jnp.logical_and(w == 0, b >= 4))
                def _():
                    for j in range(2):
                        at = j * HB + (b - 4) * 128
                        cols = pl.ds(pl.multiple_of((b - 4) * 256 + j * 128, 128), 128)
                        h, l = split(big[pl.ds(pl.multiple_of(at, 128), 128)].T)
                        lh[:, cols] = h
                        ll[:, cols] = l

                @pl.when(jnp.logical_and(w == 1, jnp.logical_and(b >= 4, b < 7)))
                def _():
                    split_g(b - 4)
            else:
                gb = b - 1

                @pl.when(jnp.logical_and(jnp.logical_or(w == g_at[0], w == g_at[1]), gb >= 0))
                def _():
                    at = jnp.where(w == g_at[1], HB, 0) + gb * 128
                    rows = pl.ds(pl.multiple_of(at, 128), 128)
                    g = split(gbuf[rows])
                    for j in range(2):
                        cols = slice(j * HB, j * HB + HB)
                        upd = mul3(g, (lh[:, cols], ll[:, cols]))
                        u[rows, cols] = u[rows, cols] - jnp.where(top, 0.0, upd)
            return 0

        lax.fori_loop(0, per * (8 if one else 5), with_update, 0)

        if one:
            split_g(3)

            def g_update(i, _):
                n, h = lax.div(i, 2), lax.rem(i, 2)
                rows = pl.ds(pl.multiple_of(h * HB, HB), HB)
                cols = pl.ds(pl.multiple_of(n * 256, 256), 256)
                upd = mul3((ph[rows], plo[rows]), (lh[:, cols], ll[:, cols]))
                for j in range(2):
                    at = pl.ds(pl.multiple_of(j * HB + n * 128, 128), 128)
                    part = jnp.where(top, 0.0, upd[:, j * 128:j * 128 + 128])
                    u[rows, at] = u[rows, at] - part
                return 0

            lax.fori_loop(0, 8, g_update, 0)
        for t in range(4):
            for s in range(2):
                @pl.when(trees[t].has[s])
                def _():
                    ref = big.at[pl.ds(0, HB)]
                    remote(ref, ref, tree_send.at[t, s], lr1.at[0], (row, col)).wait_send()
        for kind in range(3):
            ref = l10.at[pl.ds(0, HB // 2)] if kind == 1 else big.at[pl.ds(0, HB)]

            @pl.when(jnp.logical_and(zrow, on) if kind == 0 else on)
            def _():
                remote(ref, ref, zsend.at[kind, 0], lr1.at[0], (row, col)).wait_send()

            @pl.when(jnp.logical_and(zrow, row == other) if kind == 0 else far)
            def _():
                remote(ref, ref, zsend.at[kind, 1], lr1.at[0], (row, col)).wait_send()


    @pl.when(col == 1)
    def _():
        trailing(True)

    @pl.when(col > 1)
    def _():
        trailing(False)


def body(a_window, l_panel, l_inverse):
    vmem = pltpu.VMEM
    dma = pltpu.SemaphoreType.DMA
    return pl.pallas_call(
        kernel,
        out_shape=jax.ShapeDtypeStruct((W, W), F32),
        in_specs=[pl.BlockSpec(memory_space=pl.ANY)] * 2 + [pl.BlockSpec(memory_space=pltpu.VMEM)],
        out_specs=pl.BlockSpec(memory_space=pltpu.VMEM),
        scratch_shapes=[
            vmem((3 * W, W), F32),
            vmem((W, W), F32),
            vmem((HB, HB), F32),
            vmem((W, W), F32),
            vmem((W, W), BF16), vmem((W, W), BF16),
            vmem((W, W), BF16), vmem((W, W), BF16),
            vmem((W, W), BF16), vmem((W, W), BF16),
            vmem((2, HB, HB), BF16), vmem((2, HB, HB), BF16),
            vmem((2, HB, HB), BF16), vmem((2, HB, HB), BF16),
            vmem((HB, HB), BF16), vmem((HB, HB), BF16),
            vmem((HB, HB), BF16), vmem((HB, HB), BF16),
            dma((5,)),
            dma((4, 2 * KT)),
            dma((4, 2)),
            dma((4, 2)),
            dma((KZ,)), dma((KZ,)),
            dma((KZL,)), dma((KZL,)),
            dma((KZ,)), dma((KZ,)),
            dma((3, 4)),
        ],
        compiler_params=pltpu.CompilerParams(
            collective_id=0, has_side_effects=True, vmem_limit_bytes=48500000
        ),
        name="block_step",
    )(a_window, l_panel, l_inverse)


def solution(mesh):
    placed = (P("row", "col"), P("row", None), P())
    return jax.shard_map(
        body, mesh=mesh, in_specs=placed, out_specs=P("row", "col"), check_vma=False
    )
```
